32 devices in a mesh: dp: 4 (over z), row: 2 (over x), col: 4 (over y, core).
Axes of the slice: x: 2, y: 2, z: 4, core: 2. Of those that a mesh axis runs over, the one named last changes fastest.
Arguments:
- inputs: float32 [8192, 1024], P(('dp', 'row'), 'col'), may hold values from -6 to 6
- cond: float32 [8, 1024], P(('dp', 'row')), may hold values from -10 to 10
- w_ada: bfloat16 [1024, 6, 1024], P(None, None, 'col'), may hold values from -0.1875 to 0.1875
- b_ada: float32 [6, 1024], P(None, 'col'), may hold values from -3 to 3
- w_qkv: bfloat16 [3, 1024, 1024], P(None, 'col', 'row'), may hold values from -0.1875 to 0.1875
- b_qv: float32 [2, 1024], P(None, ('row', 'col')), may hold values from -3 to 3
- w_out: bfloat16 [1024, 1024], P('row', 'col'), may hold values from -0.75 to 0.75
- b_out: float32 [1024], P('col'), may hold values from -3 to 3
- w_fc1: bfloat16 [1024, 4096], P('col', 'row'), may hold values from -0.1875 to 0.1875
- b_fc1: float32 [4096], P(('row', 'col')), may hold values from -3 to 3
- w_fc2: bfloat16 [4096, 1024], P('row', 'col'), may hold values from -0.09375 to 0.09375
- b_fc2: float32 [1024], P('col'), may hold values from -5 to 5
- cotangent: float32 [8192, 1024], P(('dp', 'row'), 'col'), may hold values from -6 to 6
Outputs:
- result: float32 [8192, 1024], P(('dp', 'row'), 'col')
- grad_inputs: float32 [8192, 1024], P(('dp', 'row'), 'col')
- grad_cond: float32 [8, 1024], P(('dp', 'row'))
- grad_w_ada: float32 [1024, 6, 1024], P(None, None, 'col')
- grad_b_ada: float32 [6, 1024], P(None, 'col')
- gradient_query_key_value_weight: float32 [3, 1024, 1024], P(None, 'col', 'row')
- gradient_query_value_bias: float32 [2, 1024], P(None, ('row', 'col'))
- gradient_output_weight: float32 [1024, 1024], P('row', 'col')
- gradient_output_bias: float32 [1024], P('col')
- gradient_first_dense_weight: float32 [1024, 4096], P('col', 'row')
- gradient_first_dense_bias: float32 [4096], P(('row', 'col'))
- gradient_second_dense_weight: float32 [4096, 1024], P('row', 'col')
- gradient_second_dense_bias: float32 [1024], P('col')
The draws below stay inside these ranges and needn't reach their ends.
All inputs are finite; a program needn't handle non-finite values.
Results may differ from the reference program's by a relative error of at most 0.0131.
The reference program's roundings to bfloat16 on the way count: a program that leaves them out, or rounds other values in their place, can miss the bound.
Values may be sent and summed in bfloat16 or wider, within the bound.
A program may use at most 192 MiB of HBM per device.

```python
import jax
import jax.numpy as jnp
from jax import lax

D = 1024
HEADS = 16
HD = 64
FF = 4096
LATENT_TOKENS = 1024
NSEQ = 8
TOKENS = 8192


def draw_cond(key, part):
    first_key = jax.random.fold_in(key, 0)
    values = jax.random.normal(first_key, (NSEQ, D), jnp.float32)
    return jnp.clip(values, -10.0, 10.0)


def steps_of(stream_key, dims, cuts, smallest, high):
    def one(axis_at, shards_of):
        steps = jax.random.uniform(jax.random.fold_in(jax.random.fold_in(stream_key, 6), axis_at), (shards_of,), jnp.float32, smallest / len(cuts), high / len(cuts))
        return jnp.repeat(jnp.exp(steps), dims[axis_at] // shards_of).reshape((-1,) + (1,) * (len(dims) - axis_at - 1))

    factor_of = one(*cuts[0])
    for cut in cuts[1:]:
        factor_of = factor_of * one(*cut)
    return factor_of


def scatter_about(key, extent, width, bound, cuts=(), held_as=jnp.bfloat16):
    values = jax.random.normal(key, extent, jnp.float32) * width
    if len(cuts) > 0:
        values = steps_of(key, extent, cuts, -0.22, 0.18) * values
    return jnp.clip(values, min=-bound, max=bound).astype(held_as)


def setup_inputs(seed: int = 0) -> dict:
    splits = jax.random.split(jax.random.key(seed), 14)
    inputs = scatter_about(splits[0], (TOKENS, D), 1.0, 6.0, ((0, 8), (1, 4)), jnp.float32)
    cond = draw_cond(jax.random.fold_in(splits[13], 71), 0)
    w_ada = scatter_about(splits[2], (D, 6, D), D ** -0.5, 0.1875, ((2, 4),))
    b_ada = scatter_about(splits[3], (6, D), 0.5, 3.0, ((1, 4),), jnp.float32)
    w_qkv = scatter_about(splits[4], (3, D, D), D ** -0.5, 0.1875, ((1, 4), (2, 2)))
    b_qv = scatter_about(splits[5], (2, D), 0.5, 3.0, ((1, 8),), jnp.float32)
    w_out = scatter_about(splits[6], (D, D), (D // 16) ** -0.5, 0.75, ((0, 2), (1, 4)))
    b_out = scatter_about(splits[7], (D,), 0.5, 3.0, ((0, 4),), jnp.float32)
    w_fc1 = scatter_about(splits[8], (D, FF), D ** -0.5, 0.1875, ((0, 4), (1, 2)))
    b_fc1 = scatter_about(splits[9], (FF,), 0.5, 3.0, ((0, 8),), jnp.float32)
    w_fc2 = scatter_about(splits[10], (FF, D), FF ** -0.5, 0.09375, ((0, 2), (1, 4)))
    b_fc2 = scatter_about(splits[11], (D,), 1.0, 5.0, ((0, 4),), jnp.float32)
    cotangent = scatter_about(splits[12], (TOKENS, D), 1.0, 6.0, ((0, 8), (1, 4)), jnp.float32)
    return dict(inputs=inputs, cond=cond, w_ada=w_ada, b_ada=b_ada, w_qkv=w_qkv, b_qv=b_qv, w_out=w_out, b_out=b_out, w_fc1=w_fc1, b_fc1=b_fc1, w_fc2=w_fc2, b_fc2=b_fc2, cotangent=cotangent)


EPSILON = 1e-06

def to_low(values):
    return lax.optimization_barrier(values.astype(jnp.bfloat16))

def gelu_tanh(values):
    return jax.nn.gelu(values, approximate=True)

def moments(fields):
    average = lax.optimization_barrier(jnp.mean(fields, axis=-1, keepdims=True))
    square = lax.optimization_barrier(jnp.mean(fields * fields, axis=-1, keepdims=True))
    inverse = lax.rsqrt(square - average * average + EPSILON)
    return ((fields - average) * inverse, inverse)

def norm_back(grad_norm, normed, inverse):
    first_mean = lax.optimization_barrier(jnp.mean(grad_norm, axis=-1, keepdims=True))
    second = lax.optimization_barrier(jnp.mean(grad_norm * normed, axis=-1, keepdims=True))
    return inverse * (grad_norm - first_mean - normed * second)

def reference(inputs, cond, w_ada, b_ada, w_qkv, b_qv, w_out, b_out, w_fc1, b_fc1, w_fc2, b_fc2, cotangent):
    single_latent = jnp.float32
    factor = HD ** (-0.5)
    act_cond = jax.nn.silu(cond).astype(jnp.bfloat16)
    modulation = jnp.dot(act_cond, w_ada.reshape(D, 6 * D), preferred_element_type=single_latent).reshape(NSEQ, 6, D) + b_ada[None]
    qkv_bias = jnp.stack([b_qv[0], jnp.zeros((D,), single_latent), b_qv[1]])[:, None, :]

    def one_latent(running_totals, packed):
        latent, grad_out, mod_rows = packed
        shift_one, scale_one, gate_one = (mod_rows[0], mod_rows[1], mod_rows[2])
        shift_two, scale_two, gate_two = (mod_rows[3], mod_rows[4], mod_rows[5])
        normed_one, inverse_one = moments(latent)
        hidden_one = to_low(normed_one * (1.0 + scale_one) + shift_one)
        qkv_sum = jnp.stack([jnp.dot(hidden_one, w_qkv[member], preferred_element_type=single_latent) for member in range(3)])
        qkv_low = to_low(qkv_sum + qkv_bias)
        heads_all = qkv_low.astype(single_latent).reshape(3, LATENT_TOKENS, HEADS, HD)
        queries, keys_all, values_all = (heads_all[0], heads_all[1], heads_all[2])
        scores = jnp.einsum('qhd,khd->hqk', queries, keys_all) * factor
        log_total = jax.nn.logsumexp(scores, axis=-1)
        soft_exact = jnp.exp(scores - log_total[..., None])
        soft_weights = to_low(soft_exact).astype(single_latent)
        mixture = to_low(jnp.einsum('hqk,khd->qhd', soft_weights, values_all)).reshape(LATENT_TOKENS, D)
        mixture_wide = mixture.astype(single_latent)
        attn_out = jnp.dot(mixture, w_out, preferred_element_type=single_latent) + b_out
        middle = latent + gate_one * attn_out
        normed_two, inverse_two = moments(middle)
        hidden_two = to_low(normed_two * (1.0 + scale_two) + shift_two)
        pre_act = jnp.dot(hidden_two, w_fc1, preferred_element_type=single_latent) + b_fc1
        activated = to_low(gelu_tanh(pre_act))
        mlp_out = jnp.dot(activated, w_fc2, preferred_element_type=single_latent) + b_fc2
        result = middle + gate_two * mlp_out
        grad_mlp = grad_out * gate_two
        grad_gate_two = lax.optimization_barrier(jnp.sum(grad_out * mlp_out, axis=0))
        gradient_second_dense_bias = lax.optimization_barrier(jnp.sum(grad_mlp, axis=0))
        grad_mlp_low = to_low(grad_mlp)
        gradient_second_dense_weight = jnp.dot(activated.T, grad_mlp_low, preferred_element_type=single_latent)
        grad_act = jnp.dot(grad_mlp_low, w_fc2.T, preferred_element_type=single_latent)
        grad_pre = jax.vjp(gelu_tanh, pre_act)[1](grad_act)[0]
        gradient_first_dense_bias = lax.optimization_barrier(jnp.sum(grad_pre, axis=0))
        gradient_preactivation_local = to_low(grad_pre)
        gradient_first_dense_weight = jnp.dot(hidden_two.T, gradient_preactivation_local, preferred_element_type=single_latent)
        gradient_second_hidden = jnp.dot(gradient_preactivation_local, w_fc1.T, preferred_element_type=single_latent)
        grad_shift_two = lax.optimization_barrier(jnp.sum(gradient_second_hidden, axis=0))
        grad_scale_two = lax.optimization_barrier(jnp.sum(gradient_second_hidden * normed_two, axis=0))
        grad_middle = grad_out + norm_back(gradient_second_hidden * (1.0 + scale_two), normed_two, inverse_two)
        grad_attn = grad_middle * gate_one
        grad_gate_one = lax.optimization_barrier(jnp.sum(grad_middle * attn_out, axis=0))
        gradient_output_bias = lax.optimization_barrier(jnp.sum(grad_attn, axis=0))
        grad_attn_low = to_low(grad_attn)
        gradient_output_weight = jnp.dot(mixture.T, grad_attn_low, preferred_element_type=single_latent)
        grad_mixture = to_low(jnp.dot(grad_attn_low, w_out.T, preferred_element_type=single_latent))
        grad_heads = grad_mixture.astype(single_latent).reshape(LATENT_TOKENS, HEADS, HD)
        grad_values = jnp.einsum('hqk,qhd->khd', soft_weights, grad_heads)
        grad_soft = jnp.einsum('qhd,khd->hqk', grad_heads, values_all)
        inner_sum = lax.optimization_barrier(jnp.sum(grad_heads * mixture_wide.reshape(LATENT_TOKENS, HEADS, HD), axis=-1)).T
        grad_scores = to_low(soft_exact * (grad_soft - inner_sum[..., None])).astype(single_latent)
        grad_queries = jnp.einsum('hqk,khd->qhd', grad_scores, keys_all) * factor
        grad_keys = jnp.einsum('hqk,qhd->khd', grad_scores, queries) * factor
        grad_qkv = jnp.stack([grad_queries, grad_keys, grad_values]).reshape(3, LATENT_TOKENS, D)
        gradient_query_value_bias = jnp.stack([lax.optimization_barrier(jnp.sum(grad_qkv[0], axis=0)), lax.optimization_barrier(jnp.sum(grad_qkv[2], axis=0))])
        grad_qkv_low = to_low(grad_qkv)
        gradient_query_key_value_weight = jnp.stack([jnp.dot(hidden_one.T, grad_qkv_low[member], preferred_element_type=single_latent) for member in range(3)])
        grad_hidden_one = jnp.einsum('kle,kde->ld', grad_qkv_low.astype(single_latent), w_qkv.astype(single_latent))
        grad_shift_one = lax.optimization_barrier(jnp.sum(grad_hidden_one, axis=0))
        grad_scale_one = lax.optimization_barrier(jnp.sum(grad_hidden_one * normed_one, axis=0))
        grad_inputs = grad_middle + norm_back(grad_hidden_one * (1.0 + scale_one), normed_one, inverse_one)
        grad_modulation = jnp.stack([grad_shift_one, grad_scale_one, grad_gate_one, grad_shift_two, grad_scale_two, grad_gate_two])
        summand_terms = (gradient_query_key_value_weight, gradient_query_value_bias, gradient_output_weight, gradient_output_bias, gradient_first_dense_weight, gradient_first_dense_bias, gradient_second_dense_weight, gradient_second_dense_bias)
        running_totals = jax.tree.map(lambda prior_value, apply_update: prior_value + apply_update, running_totals, summand_terms)
        return (running_totals, (result, grad_inputs, grad_modulation))
    initial = (jnp.zeros((3, D, D), single_latent), jnp.zeros((2, D), single_latent), jnp.zeros((D, D), single_latent), jnp.zeros((D,), single_latent), jnp.zeros((D, FF), single_latent), jnp.zeros((FF,), single_latent), jnp.zeros((FF, D), single_latent), jnp.zeros((D,), single_latent))
    packed_all = (inputs.reshape(NSEQ, LATENT_TOKENS, D), cotangent.reshape(NSEQ, LATENT_TOKENS, D), modulation)
    running_totals, outputs = lax.scan(one_latent, initial, packed_all)
    results, grad_inputs, grad_modulation = outputs
    gradient_query_key_value_weight, gradient_query_value_bias, gradient_output_weight, gradient_output_bias, gradient_first_dense_weight, gradient_first_dense_bias, gradient_second_dense_weight, gradient_second_dense_bias = running_totals
    grad_mod_flat = grad_modulation.reshape(NSEQ, 6 * D)
    grad_w_ada = jnp.dot(act_cond.astype(single_latent).T, grad_mod_flat, precision=lax.Precision.HIGHEST, preferred_element_type=single_latent).reshape(D, 6, D)
    grad_b_ada = lax.optimization_barrier(jnp.sum(grad_modulation, axis=0))
    grad_silu = jnp.dot(grad_mod_flat, w_ada.astype(single_latent).reshape(D, 6 * D).T, precision=lax.Precision.HIGHEST, preferred_element_type=single_latent)
    grad_cond = jax.vjp(jax.nn.silu, cond)[1](grad_silu)[0]
    return (results.reshape(TOKENS, D), grad_inputs.reshape(TOKENS, D), grad_cond, grad_w_ada, grad_b_ada, gradient_query_key_value_weight, gradient_query_value_bias, gradient_output_weight, gradient_output_bias, gradient_first_dense_weight, gradient_first_dense_bias, gradient_second_dense_weight, gradient_second_dense_bias)
```

```python
import functools

import jax
import jax.numpy as jnp
from jax import lax
from jax.experimental import pallas as pl
from jax.experimental.pallas import tpu as pltpu
from jax.sharding import PartitionSpec as P

D = 1024
HD = 64
T = 1024
EPSILON = 1e-06
bf16, f32 = jnp.bfloat16, jnp.float32
MESH = pl.DeviceIdType.MESH
NN = ((1,), (0,))
NT = ((1,), (1,))
TN = ((0,), (0,))
FACTOR = HD ** (-0.5)
LOG2E = 1.4426950408889634
GC = 0.7978845608028654
N_SEM = 256


def dot(a, b, dims):
    return lax.dot_general(a, b, (dims, ((), ())), preferred_element_type=f32)


def loop(count, step):
    def one(i, carry):
        step(i)
        return carry

    lax.fori_loop(0, count, one, 0)


def at(start, size):
    if isinstance(start, int):
        return pl.ds(start, size)
    return pl.ds(pl.multiple_of(start, size), size)


def rows_of(i, size):
    return at(i * size, size)


def mega(
    ndp,
    x_hbm,
    cot_hbm,
    wqkv,
    wout,
    wfc1,
    wfc2,
    mod,
    actb,
    bqv,
    bout,
    bfc1,
    bfc2,
    res_o,
    gin_o,
    gq_o,
    go_o,
    g1_o,
    g2_o,
    gm_o,
    act_o,
    gmo_o,
    gbqv_o,
    gbfc1_o,
    gbout_o,
    gbfc2_o,
    gbada_o,
    X,
    COT,
    N1,
    N2,
    ATT,
    WQ,
    WOUT,
    WF1,
    WF2,
    H1,
    MIX,
    H2,
    GM,
    Q,
    K,
    V,
    KT,
    LT,
    L8,
    I8,
    GA,
    DO,
    ACT,
    GPRE,
    SA,
    SAR,
    YA,
    YAR,
    SB,
    SBR,
    YB,
    YBR,
    SC,
    SCR,
    YC,
    YCR,
    ACCA,
    ACCB,
    DQT,
    DK,
    DV,
    QM,
    DOM,
    GQKV,
    X1S,
    X1R,
    ZS1,
    ZR1,
    A1,
    X2S,
    X2R,
    ZS2,
    ZR2,
    A2,
    XQS,
    XQR,
    ZSQ,
    ZRQ,
    AQ,
    XOS,
    XOR,
    ZSO,
    ZRO,
    AO,
    ST,
    CV,
    SBX,
    SVL,
    SVA,
    ACA,
    ss,
    rs,
    ls,
):
    nl = 2 * ndp
    d, r, c = lax.axis_index("dp"), lax.axis_index("row"), lax.axis_index("col")
    me = d * 2 + r
    sib, yc, dg = c + 1 - 2 * (c % 2), (c + 2) % 4, 3 - c
    dev_s, dev_y, dev_g, dev_x = (d, r, sib), (d, r, yc), (d, r, dg), (d, 1 - r, c)
    q_ = 1 - r

    count = [0, 0]

    def sem(k=1):
        base = count[0]
        count[0] += k
        assert count[0] <= ss.shape[0]
        return base

    def lsem(k=1):
        base = count[1]
        count[1] += k
        assert count[1] <= ls.shape[0]
        return base

    def rc(src, dst, i, dev):
        return pltpu.make_async_remote_copy(
            src_ref=src,
            dst_ref=dst,
            send_sem=ss.at[i],
            recv_sem=rs.at[i],
            device_id=dev,
            device_id_type=MESH,
        )

    def lc(src, dst, i):
        return pltpu.make_async_copy(src, dst, ls.at[i])

    finals = []

    lane256 = lax.broadcasted_iota(jnp.int32, (256, 256), 1) // HD
    lane128 = lax.broadcasted_iota(jnp.int32, (128, 128), 1)

    cx, ccot = lc(x_hbm, X, lsem()), lc(cot_hbm, COT, lsem())
    cx.start()
    ccot.start()
    barrier = pltpu.get_barrier_semaphore()
    for dev in (dev_s, dev_y, dev_g):
        pl.semaphore_signal(barrier, inc=1, device_id=dev, device_id_type=MESH)

    def greet(o):
        other = (me + o + 1) % nl
        pl.semaphore_signal(
            barrier, inc=1, device_id=(other // 2, other % 2, c), device_id_type=MESH
        )

    loop(nl - 1, greet)
    pl.semaphore_wait(barrier, nl + 2)

    class Weight:
        def __init__(self, src, dst):
            self.src, self.dst = src, dst
            self.a, self.x, self.l = sem(4), sem(4), lsem()

        def start(self):
            self.local = lc(self.src(c), self.dst(c, r), self.l)
            self.local.start()
            for off in (2, 3, 1):
                to = (c + off) % 4
                cp = rc(self.src(to), self.dst(c, r), self.a + off, (d, r, to))
                cp.start()
                finals.append(cp.wait_send)
            cp = rc(self.src(c), self.dst(c, r), self.x, dev_x)
            cp.start()
            finals.append(cp.wait_send)

        def forward(self, off):
            cs = (c + 4 - off) % 4
            here = self.dst(cs, r)
            rc(here, here, self.a + off, dev_s).wait_recv()
            cp = rc(here, here, self.x + off, dev_x)
            cp.start()
            finals.append(cp.wait_send)

        def wait(self):
            self.local.wait()
            for off in range(4):
                there = self.dst((c + 4 - off) % 4, q_)
                rc(there, there, self.x + off, dev_x).wait_recv()

    w_qkv = Weight(
        lambda c2: wqkv.at[:, :, at(c2 * 128, 128)],
        lambda cs, ro: WQ.at[:, at(cs * 256, 256), at(ro * 128, 128)],
    )
    w_fc1 = Weight(
        lambda c2: wfc1.at[:, at(c2 * 512, 512)],
        lambda cs, ro: WF1.at[at(cs * 256, 256), at(ro * 512, 512)],
    )
    w_fc2 = Weight(
        lambda c2: wfc2.at[at(c2 * 512, 512), :],
        lambda cs, ro: WF2.at[at(ro * 512, 512), at(cs * 256, 256)],
    )
    w_qkv.start()

    SBX[r, 0:1, :] = bfc1[...]
    SBX[r, 1:2, 0:128] = bqv[0:1, :]
    SBX[r, 1:2, 128:256] = bqv[1:2, :]
    sbx = sem()
    cp = rc(SBX.at[r], SBX.at[r], sbx, dev_x)
    cp.start()
    finals.append(cp.wait_send)

    wo, wol = sem(4), lsem(4)
    for cs in range(4):
        place = WOUT.at[at(256 * cs + 128 * r, 128), :]
        cp = rc(wout.at[at(cs * 128, 128), :], place, wo + cs, dev_x)
        cp.start()
        finals.append(cp.wait_send)
        lc(wout.at[at(cs * 128, 128), :], place, wol + cs).start()

    def wait_wout():
        for cs in range(4):
            place = WOUT.at[at(256 * cs + 128 * r, 128), :]
            lc(wout.at[at(cs * 128, 128), :], place, wol + cs).wait()
            there = WOUT.at[at(256 * cs + 128 * q_, 128), :]
            rc(there, there, wo + cs, dev_x).wait_recv()

    class ToAll:
        def __init__(self, buf):
            self.buf, self.s = buf, sem(nl - 1)

        def start(self):
            def one(o):
                other = (me + o + 1) % nl
                rc(self.buf.at[me], self.buf.at[me], self.s + o, (other // 2, other % 2, c)).start()

            loop(nl - 1, one)

        def wait(self):
            def one(o):
                other = (me + nl - o - 1) % nl
                rc(self.buf.at[other], self.buf.at[other], self.s + o, dev_x).wait()

            loop(nl - 1, one)

    class Gather:
        def __init__(self, buf):
            self.buf, self.s = buf, sem(12)
            finals.append(lambda: loop(4, self.drain))

        def reg(self, i, cs):
            return self.buf.at[rows_of(i, 256), at(cs * 256, 256)]

        def start(self, i):
            mine = self.reg(i, c)
            rc(mine, mine, self.s + i, dev_y).start()
            rc(mine, mine, self.s + 4 + i, dev_s).start()

        def forward(self, i):
            theirs = self.reg(i, yc)
            rc(theirs, theirs, self.s + i, dev_y).wait_recv()
            rc(theirs, theirs, self.s + 8 + i, dev_s).start()

        def wait(self, i):
            a, b = self.reg(i, sib), self.reg(i, dg)
            rc(a, a, self.s + 4 + i, dev_s).wait_recv()
            rc(b, b, self.s + 8 + i, dev_s).wait_recv()

        def drain(self, i):
            mine, theirs = self.reg(i, c), self.reg(i, yc)
            rc(mine, mine, self.s + i, dev_y).wait_send()
            rc(mine, mine, self.s + 4 + i, dev_s).wait_send()
            rc(theirs, theirs, self.s + 8 + i, dev_s).wait_send()

    class Scatter:
        def __init__(self, part, snd, srec, ysnd, yrec, acc):
            self.part, self.snd, self.srec = part, snd, srec
            self.ysnd, self.yrec, self.acc = ysnd, yrec, acc
            self.s = sem(8)

        def one(self, i):
            rows = rows_of(i, 256)
            self.snd[rows, 0:256] = self.part(i, dg).astype(bf16)
            self.snd[rows, 256:512] = self.part(i, sib).astype(bf16)
            rc(self.snd.at[rows], self.srec.at[rows], self.s + i, dev_s).start()

        def two(self, i):
            rows = rows_of(i, 256)
            value = self.part(i, yc)
            rc(self.snd.at[rows], self.srec.at[rows], self.s + i, dev_s).wait_recv()
            self.ysnd[rows, :] = (value + self.srec[rows, 0:256].astype(f32)).astype(bf16)
            rc(self.ysnd.at[rows], self.yrec.at[rows], self.s + 4 + i, dev_y).start()

        def three(self, i):
            rows = rows_of(i, 256)
            self.acc[rows, :] = self.part(i, c) + self.srec[rows, 256:512].astype(f32)

        def four(self, i):
            rows = rows_of(i, 256)
            rc(self.ysnd.at[rows], self.yrec.at[rows], self.s + 4 + i, dev_y).wait_recv()
            return self.acc[rows, :] + self.yrec[rows, :].astype(f32)

        def drain(self):
            def one(i):
                rows = rows_of(i, 256)
                rc(self.snd.at[rows], self.srec.at[rows], self.s + i, dev_s).wait_send()
                rc(self.ysnd.at[rows], self.yrec.at[rows], self.s + 4 + i, dev_y).wait_send()

            loop(4, one)

        def launch(self):
            loop(4, self.one)
            loop(4, self.two)
            loop(4, self.three)

    class Stats:
        def __init__(self, e):
            self.e, self.s = e, sem(3)

        def put(self, i, a, b):
            both = jnp.where(lane128 == 0, a, jnp.where(lane128 == 1, b, 0.0)).T
            ST[self.e, c, pl.ds(i, 1), :] = both[0:1, :]
            ST[self.e, c, pl.ds(8 + i, 1), :] = both[1:2, :]

        def exchange(self):
            mine = ST.at[self.e, c]
            for n, dev in enumerate((dev_s, dev_y, dev_g)):
                cp = rc(mine, mine, self.s + n, dev)
                cp.start()
                finals.append(cp.wait_send)

        def total(self):
            for n, (dev, cs) in enumerate(((dev_s, sib), (dev_y, yc), (dev_g, dg))):
                there = ST.at[self.e, cs]
                rc(there, there, self.s + n, dev).wait_recv()
            total = ST[self.e, 0] + ST[self.e, 1] + ST[self.e, 2] + ST[self.e, 3]
            return total[0:8, :], total[8:16, :]

    def column(n, i):
        half = jnp.broadcast_to(CV[n, pl.ds(i, 1), :], (128, 128)).T
        return jnp.concatenate([half, half], axis=1)

    def token_sum(value):
        return jnp.sum(value, axis=0, keepdims=True)

    row_shift1, row_scale1, row_gate1 = mod[0:1, :], 1.0 + mod[1:2, :], mod[2:3, :]
    row_shift2, row_scale2, row_gate2 = mod[3:4, :], 1.0 + mod[4:5, :], mod[5:6, :]
    mine = at(256 * c, 256)
    SVL[...] = jnp.zeros_like(SVL)
    G_SHIFT1, G_SCALE1, G_GATE1 = (2, 0), (2, 256), (3, 0)
    G_SHIFT2, G_SCALE2, G_GATE2 = (3, 256), (4, 0), (4, 256)

    def add_to(where, value):
        row, lane = where
        SVL[row : row + 1, lane : lane + value.shape[1]] += value

    ACA[me] = actb[...]
    aca = ToAll(ACA)
    aca.start()
    st1, st2, st3, st4 = Stats(0), Stats(1), Stats(2), Stats(3)
    cx.wait()

    def n1_sums(i):
        x = X[rows_of(i, 128), :]
        st1.put(i, jnp.sum(x, axis=1, keepdims=True), jnp.sum(x * x, axis=1, keepdims=True))

    loop(8, n1_sums)
    st1.exchange()
    ccot.wait()

    def gm_step(i):
        rows = rows_of(i, 128)
        g = COT[rows, :] * row_gate2
        add_to((6, 256), token_sum(g))
        GM[rows, mine] = g.astype(bf16)

    loop(8, gm_step)
    s1, s2 = st1.total()
    average = s1 / D
    CV[0] = average
    CV[1] = lax.rsqrt(s2 / D - average * average + EPSILON)
    ag_h1, ag_mix, ag_h2, ag_gm = Gather(H1), Gather(MIX), Gather(H2), Gather(GM)

    def n1_norm(i):
        for s in range(2):
            rows = at(i * 256 + s * 128, 128)
            normed = (X[rows, :] - column(0, 2 * i + s)) * column(1, 2 * i + s)
            N1[rows, :] = normed
            H1[rows, mine] = (normed * row_scale1 + row_shift1).astype(bf16)
        ag_h1.start(i)

    loop(4, n1_norm)
    for off in (1, 2, 3):
        w_qkv.forward(off)
    loop(4, ag_h1.forward)
    w_fc1.start()

    there = SBX.at[q_]
    rc(there, there, sbx, dev_x).wait_recv()
    w_qkv.wait()

    def qkv_step(i):
        ag_h1.wait(i)
        rows = rows_of(i, 256)
        h = H1[rows, :]
        qb = jnp.concatenate([SBX[0, 1:2, 0:128], SBX[1, 1:2, 0:128]], axis=1)
        vb = jnp.concatenate([SBX[0, 1:2, 128:256], SBX[1, 1:2, 128:256]], axis=1)
        Q[rows, :] = (dot(h, WQ[0], NN) + qb).astype(bf16)
        K[rows, :] = dot(h, WQ[1], NN).astype(bf16)
        V[rows, :] = (dot(h, WQ[2], NN) + vb).astype(bf16)

    loop(4, qkv_step)

    def att_step(i):
        rows = rows_of(i, 256)
        qt = Q[rows, :]
        out = jnp.zeros((256, 256), f32)
        logs = jnp.zeros((256, 128), f32)
        lane = lax.broadcasted_iota(jnp.int32, (256, 128), 1)
        for h in range(4):
            qm = jnp.where(lane256 == h, qt, jnp.zeros_like(qt))
            s = dot(qm, K[...], NT)
            m = jnp.max(s, axis=1, keepdims=True)
            p = jnp.exp2((s - m) * (FACTOR * LOG2E))
            total = jnp.sum(p, axis=1, keepdims=True)
            o = dot(p.astype(bf16), V[...], NN)
            out = jnp.where(lane256 == h, o / total, out)
            logs = jnp.where(lane == h, m * (FACTOR * LOG2E) + jnp.log2(total), logs)
        MIX[rows, mine] = out.astype(bf16)
        LT[rows, :] = logs
        ag_mix.start(i)

        @pl.when(i >= 2)
        def _():
            ag_mix.forward(i - 2)

    loop(4, att_step)
    for off in (1, 2, 3):
        w_fc1.forward(off)
    ag_mix.forward(2)
    ag_mix.forward(3)
    w_fc2.start()
    loop(4, ag_gm.start)

    wait_wout()

    def out_step(i):
        ag_mix.wait(i)
        rows = rows_of(i, 256)
        att = dot(MIX[rows, :], WOUT[...], NN) + bout[...]
        ATT[rows, :] = att
        X[rows, :] = X[rows, :] + row_gate1 * att

    loop(4, out_step)

    def n2_sums(i):
        x = X[rows_of(i, 128), :]
        st2.put(i, jnp.sum(x, axis=1, keepdims=True), jnp.sum(x * x, axis=1, keepdims=True))

    loop(8, n2_sums)
    st2.exchange()
    s1, s2 = st2.total()
    average = s1 / D
    CV[2] = average
    CV[3] = lax.rsqrt(s2 / D - average * average + EPSILON)

    def n2_norm(i):
        for s in range(2):
            rows = at(i * 256 + s * 128, 128)
            normed = (X[rows, :] - column(2, 2 * i + s)) * column(3, 2 * i + s)
            N2[rows, :] = normed
            H2[rows, mine] = (normed * row_scale2 + row_shift2).astype(bf16)
        ag_h2.start(i)

    loop(4, n2_norm)
    for off in (1, 2, 3):
        w_fc2.forward(off)
    loop(4, ag_gm.forward)
    loop(4, ag_h2.forward)
    w_fc1.wait()
    w_fc2.wait()

    def mlp_step(i):
        ag_gm.wait(i)
        ag_h2.wait(i)
        rows = rows_of(i, 256)
        for j in range(2):
            units = slice(512 * j, 512 * j + 512)
            v = dot(H2[rows, :], WF1[:, units], NN) + SBX[j, 0:1, :]
            g = dot(GM[rows, :], WF2[units, :], NT)
            sq = v * v
            t = jnp.tanh(GC * v * (1.0 + 0.044715 * sq))
            half = 0.5 * (1.0 + t)
            ACT[rows, units] = (v * half).astype(bf16)
            slope = half + (0.5 * GC) * v * (1.0 - t * t) * (1.0 + (3 * 0.044715) * sq)
            g = g * slope
            add_to((j, 0), token_sum(g))
            GPRE[rows, units] = g.astype(bf16)

    loop(4, mlp_step)

    rs_h2 = Scatter(
        lambda i, b: dot(GPRE[rows_of(i, 256), :], WF1[at(b * 256, 256), :], NT),
        SA, SAR, YA, YAR, ACCA,
    )
    rs_h2.launch()

    x1, x2, xq, xo = sem(4), sem(2), sem(4), sem()

    def dw1_step(i):
        h = H2[:, rows_of(i, 256)]
        X1S[i] = dot(h, GPRE[:, at(512 * q_, 512)], TN).astype(bf16)
        rc(X1S.at[i], X1R.at[i], x1 + i, dev_x).start()
        ZS1[i] = dot(h, GPRE[:, at(512 * r, 512)], TN).astype(bf16)

    loop(4, dw1_step)

    rs_out = Scatter(
        lambda i, b: dot(ACT[rows_of(i, 256), :], WF2[:, at(b * 256, 256)], NN),
        SB, SBR, YB, YBR, ACCB,
    )
    rs_out.launch()

    def dw2_step(i):
        rows = rows_of(i, 256)
        X2S[rows, :] = dot(ACT[:, at(512 * q_ + 256 * i, 256)], GM[...], TN).astype(bf16)
        rc(X2S.at[rows], X2R.at[rows], x2 + i, dev_x).start()
        ZS2[rows, :] = dot(ACT[:, at(512 * r + 256 * i, 256)], GM[...], TN).astype(bf16)

    loop(2, dw2_step)

    def b2_sums(i):
        value = rs_h2.four(i)
        ACCA[rows_of(i, 256), :] = value
        for s in range(2):
            rows = at(i * 256 + s * 128, 128)
            gh, normed = ACCA[rows, :], N2[rows, :]
            add_to(G_SHIFT2, token_sum(gh))
            hn = gh * normed
            add_to(G_SCALE2, token_sum(hn))
            st3.put(
                2 * i + s,
                jnp.sum(gh * row_scale2, axis=1, keepdims=True),
                jnp.sum(hn * row_scale2, axis=1, keepdims=True),
            )

    loop(4, b2_sums)
    st3.exchange()
    s1, s2 = st3.total()
    CV[4] = s1 / D
    CV[5] = s2 / D

    def b2_back(i):
        rows = rows_of(i, 128)
        inner = ACCA[rows, :] * row_scale2 - column(4, i) - N2[rows, :] * column(5, i)
        gmid = COT[rows, :] + column(3, i) * inner
        COT[rows, :] = gmid
        ga = gmid * row_gate1
        add_to((6, 0), token_sum(ga))
        add_to(G_GATE1, token_sum(gmid * ATT[rows, :]))
        GA[rows, :] = ga.astype(bf16)

    def out_done(i):
        value = rs_out.four(i) + bfc2[...]
        rows = rows_of(i, 256)
        add_to(G_GATE2, token_sum(COT[rows, :] * value))
        res_o[rows, :] = X[rows, :] + row_gate2 * value

    loop(4, out_done)
    loop(8, b2_back)
    rs_mix = Scatter(
        lambda i, b: dot(GA[rows_of(i, 256), :], WOUT[at(b * 256, 256), :], NT),
        SC, SCR, YC, YCR, ACCA,
    )
    rs_mix.launch()

    def dwo_step(i):
        rows = rows_of(i, 128)
        XOS[rows, :] = dot(MIX[:, at(256 * i + 128 * q_, 128)], GA[...], TN).astype(bf16)
        ZSO[rows, :] = dot(MIX[:, at(256 * i + 128 * r, 128)], GA[...], TN).astype(bf16)

    loop(4, dwo_step)
    rc(XOS, XOR, xo, dev_x).start()

    n1, n2 = 256 // ndp, 512 // ndp
    s_z1, s_z2, s_zq, s_zo = sem(ndp - 1), sem(ndp - 1), sem(ndp - 1), sem(ndp - 1)
    s_a1, s_a2, s_aq = sem(4), sem(4), sem(4)
    l_a1, l_a2, l_aq, l_ao = lsem(), lsem(), lsem(), lsem()
    s_g1, s_g2, s_gq, s_go = sem(ndp - 1), sem(ndp - 1), sem(ndp - 1), sem(ndp - 1)

    def zsend(sets):
        def one(o):
            z = (d + o + 1) % ndp
            for cut, slot, s in sets:
                rc(cut(z), slot(o), s + o, (z, r, c)).start()

        loop(ndp - 1, one)

    def zrecv(sets):
        def one(o):
            z = (d + o + 1) % ndp
            for cut, slot, s in sets:
                rc(cut(z), slot(o), s + o, (z, r, c)).wait()

        loop(ndp - 1, one)

    z1 = (lambda z: ZS1.at[:, at(z * n1, n1), :], lambda o: ZR1.at[o], s_z1)
    z2 = (lambda z: ZS2.at[at(z * n2, n2), :], lambda o: ZR2.at[o], s_z2)
    zq = (lambda z: ZSQ.at[:, :, at(z * n1, n1), :], lambda o: ZRQ.at[o], s_zq)
    zo = (lambda z: ZSO.at[at(z * n2, n2), :], lambda o: ZRO.at[o], s_zo)

    def spread(src, dst, s, l):
        lc(src(c), dst(c), l).start()
        for off in (1, 2, 3):
            to = (c + off) % 4
            cp = rc(src(to), dst(c), s + off, (d, r, to))
            cp.start()
            finals.append(cp.wait_send)

    def spread_wait(src, dst, s, l):
        lc(src(c), dst(c), l).wait()
        for off in (1, 2, 3):
            there = dst((c + 4 - off) % 4)
            rc(there, there, s + off, dev_s).wait_recv()

    sp1 = (lambda c2: A1.at[c2], lambda cs: g1_o.at[at(d * n1, n1), at(512 * cs, 512)], s_a1, l_a1)
    sp2 = (lambda c2: A2.at[:, at(256 * c2, 256)], lambda cs: g2_o.at[cs, at(d * n2, n2), :], s_a2, l_a2)
    spq = (
        lambda c2: AQ.at[c2],
        lambda cs: gq_o.at[:, at(d * n1, n1), at(128 * cs, 128)],
        s_aq,
        l_aq,
    )

    def zspread(sets):
        def one(o):
            z = (d + o + 1) % ndp
            for cut, s in sets:
                rc(cut(d), cut(d), s + o, (z, r, c)).start()

        loop(ndp - 1, one)

        def done(o):
            z = (d + ndp - o - 1) % ndp
            for cut, s in sets:
                rc(cut(z), cut(z), s + o, (z, r, c)).wait()

        finals.append(lambda: loop(ndp - 1, done))

    ag1 = (lambda z: g1_o.at[at(z * n1, n1), :], s_g1)
    ag2 = (lambda z: g2_o.at[:, at(z * n2, n2), :], s_g2)
    agq = (lambda z: gq_o.at[:, at(z * n1, n1), :], s_gq)
    ago = (lambda z: go_o.at[at(z * n2, n2), :], s_go)

    def x1_step(i):
        rc(X1S.at[i], X1R.at[i], x1 + i, dev_x).wait()
        ZS1[i] = (ZS1[i].astype(f32) + X1R[i].astype(f32)).astype(bf16)

    def x2_step(i):
        rows = rows_of(i, 256)
        rc(X2S.at[rows], X2R.at[rows], x2 + i, dev_x).wait()
        ZS2[rows, :] = (ZS2[rows, :].astype(f32) + X2R[rows, :].astype(f32)).astype(bf16)

    loop(4, x1_step)
    zsend([z1])
    loop(2, x2_step)
    zsend([z2])

    def do_step(i):
        DO[rows_of(i, 256), :] = rs_mix.four(i).astype(bf16)

    loop(4, do_step)

    def inner_step(i):
        rows = rows_of(i, 128)
        prod = DO[rows, :].astype(f32) * MIX[rows, mine].astype(f32)
        lane = lax.broadcasted_iota(jnp.int32, (128, 256), 1) // HD
        inner = jnp.zeros((128, 128), f32)
        for h in range(4):
            one = jnp.sum(jnp.where(lane == h, prod, 0.0), axis=1, keepdims=True)
            inner = jnp.where(lane128 == h, one, inner)
        I8[:, rows] = inner.T[0:8, :]
        L8[:, rows] = LT[rows, :].T[0:8, :]

    loop(8, inner_step)

    def kt_step(i):
        rows = rows_of(i, 256)
        KT[:, rows] = K[rows, :].astype(f32).T.astype(bf16)

    loop(4, kt_step)
    DQT[...] = jnp.zeros_like(DQT)
    lane_all = lax.broadcasted_iota(jnp.int32, (1024, 256), 1) // HD

    def head_back(h):
        QM[...] = jnp.where(lane_all == h, Q[...], jnp.zeros_like(Q[...]))
        DOM[...] = jnp.where(lane_all == h, DO[...], jnp.zeros_like(DO[...]))
        lrow, irow = L8[h : h + 1, :], I8[h : h + 1, :]

        def step(i):
            rows = rows_of(i, 512)
            p = jnp.exp2(dot(K[rows, :], QM[...], NT) * (FACTOR * LOG2E) - lrow)
            dp = dot(V[rows, :], DOM[...], NT)
            ds = (p * (dp - irow)).astype(bf16)
            gv, gk = dot(p.astype(bf16), DOM[...], NN), dot(ds, QM[...], NN)
            if h == 0:
                DV[rows, :] = gv
                DK[rows, :] = gk
            else:
                DV[rows, :] += gv
                DK[rows, :] += gk
            DQT[h * HD : (h + 1) * HD, :] += dot(KT[h * HD : (h + 1) * HD, rows], ds, NN)

        loop(2, step)

    head_back(0)
    head_back(1)
    zrecv([z1])
    total = ZS1[:, at(d * n1, n1), :].astype(f32)
    for o in range(ndp - 1):
        total = total + ZR1[o].astype(f32)
    A1[...] = total.astype(bf16)
    spread(*sp1)
    head_back(2)
    spread_wait(*sp1)
    zspread([ag1])
    head_back(3)
    zrecv([z2])
    total = ZS2[at(d * n2, n2), :].astype(f32)
    for o in range(ndp - 1):
        total = total + ZR2[o].astype(f32)
    A2[...] = total.astype(bf16)
    spread(*sp2)

    def gqkv_step(i):
        rows = rows_of(i, 256)
        gq = DQT[:, rows].T * FACTOR
        gk, gv = DK[rows, :] * FACTOR, DV[rows, :]
        add_to((5, 0), token_sum(gq))
        add_to((5, 256), token_sum(gv))
        GQKV[0, rows, :] = gq.astype(bf16)
        GQKV[1, rows, :] = gk.astype(bf16)
        GQKV[2, rows, :] = gv.astype(bf16)

    loop(4, gqkv_step)

    def part_h1(i, b):
        rows, feats = rows_of(i, 256), at(b * 256, 256)
        total = dot(GQKV[0, rows, :], WQ[0, feats, :], NT)
        total = total + dot(GQKV[1, rows, :], WQ[1, feats, :], NT)
        return total + dot(GQKV[2, rows, :], WQ[2, feats, :], NT)

    rs_h2.drain()
    rs_h1 = Scatter(part_h1, SA, SAR, YA, YAR, ACCB)
    loop(4, rs_h1.one)
    loop(4, rs_h1.two)

    def dwq_step(i):
        h = H1[:, rows_of(i, 256)]
        for j in range(3):
            t = dot(h, GQKV[j], TN)
            low, high = t[:, 0:128], t[:, 128:256]
            XQS[i, j] = jnp.where(r == 0, high, low).astype(bf16)
            ZSQ[i, j] = jnp.where(r == 0, low, high).astype(bf16)
        rc(XQS.at[i], XQR.at[i], xq + i, dev_x).start()

    loop(4, dwq_step)
    loop(4, rs_h1.three)
    spread_wait(*sp2)
    zspread([ag2])
    rc(XOS, XOR, xo, dev_x).wait()
    ZSO[...] = (ZSO[...].astype(f32) + XOR[...].astype(f32)).astype(bf16)
    zsend([zo])

    def b1_sums(i):
        value = rs_h1.four(i)
        ACCB[rows_of(i, 256), :] = value
        for s in range(2):
            rows = at(i * 256 + s * 128, 128)
            gh, normed = ACCB[rows, :], N1[rows, :]
            add_to(G_SHIFT1, token_sum(gh))
            hn = gh * normed
            add_to(G_SCALE1, token_sum(hn))
            st4.put(
                2 * i + s,
                jnp.sum(gh * row_scale1, axis=1, keepdims=True),
                jnp.sum(hn * row_scale1, axis=1, keepdims=True),
            )

    loop(4, b1_sums)
    st4.exchange()
    SVA[me] = SVL[...]
    sva = ToAll(SVA)
    sva.start()

    def xq_step(i):
        rc(XQS.at[i], XQR.at[i], xq + i, dev_x).wait()
        ZSQ[i] = (ZSQ[i].astype(f32) + XQR[i].astype(f32)).astype(bf16)

    loop(4, xq_step)
    zsend([zq])
    s1, s2 = st4.total()
    CV[6] = s1 / D
    CV[7] = s2 / D

    def b1_back(i):
        rows = rows_of(i, 128)
        inner = ACCB[rows, :] * row_scale1 - column(6, i) - N1[rows, :] * column(7, i)
        gin_o[rows, :] = COT[rows, :] + column(1, i) * inner

    loop(8, b1_back)

    zrecv([zo])
    total = ZSO[at(d * n2, n2), :].astype(f32)
    for o in range(ndp - 1):
        total = total + ZRO[o].astype(f32)
    AO[...] = total.astype(bf16)
    lc(AO, go_o.at[at(d * n2, n2), :], l_ao).start()
    zrecv([zq])
    total = ZSQ[:, :, at(d * n1, n1), :].astype(f32)
    for o in range(ndp - 1):
        total = total + ZRQ[o].astype(f32)
    AQ[...] = total.astype(bf16)
    spread(*spq)
    lc(AO, go_o.at[at(d * n2, n2), :], l_ao).wait()
    zspread([ago])
    spread_wait(*spq)
    zspread([agq])

    aca.wait()
    sva.wait()
    total = jnp.zeros((8, 512), f32)
    for l in range(nl):
        one = SVA[l]
        total = total + one
        act_o[l : l + 1, :] = ACA[l, 0:1, :]
        for k in range(6):
            gm_o[l, k : k + 1, :] = one[2 + k // 2 : 3 + k // 2, 256 * (k % 2) : 256 * (k % 2) + 256]
        gm_o[l, 6:8, :] = jnp.zeros((2, 256), f32)
    gmo_o[...] = gm_o[me]
    first = r == 0
    for k in range(6):
        gbada_o[k : k + 1, :] = total[2 + k // 2 : 3 + k // 2, 256 * (k % 2) : 256 * (k % 2) + 256]
    gbfc1_o[...] = jnp.where(first, total[0:1, :], total[1:2, :])
    gbqv_o[0:1, :] = jnp.where(first, total[5:6, 0:128], total[5:6, 128:256])
    gbqv_o[1:2, :] = jnp.where(first, total[5:6, 256:384], total[5:6, 384:512])
    gbout_o[...] = total[6:7, 0:256]
    gbfc2_o[...] = total[6:7, 256:512]

    rs_out.drain()
    rs_mix.drain()
    rs_h1.drain()
    for one in finals:
        one()


def call_mega(ndp, *args):
    nl = 2 * ndp
    n1, n2 = 256 // ndp, 512 // ndp
    s = jax.ShapeDtypeStruct
    vmem = pl.BlockSpec(memory_space=pltpu.VMEM)
    hbm = pl.BlockSpec(memory_space=pl.ANY)
    outs = (
        (s((T, 256), f32), vmem),
        (s((T, 256), f32), vmem),
        (s((3, 256, 512), bf16), hbm),
        (s((512, 256), bf16), hbm),
        (s((256, 2048), bf16), hbm),
        (s((4, 512, 256), bf16), hbm),
        (s((nl, 8, 256), f32), vmem),
        (s((nl, D), f32), vmem),
        (s((8, 256), f32), vmem),
        (s((2, 128), f32), vmem),
        (s((1, 512), f32), vmem),
        (s((1, 256), f32), vmem),
        (s((1, 256), f32), vmem),
        (s((6, 256), f32), vmem),
    )

    def v(*shape, t=bf16):
        return pltpu.VMEM(shape, t)

    scratch = (
        [v(T, 256, t=f32)] * 5
        + [v(3, D, 256), v(D, 256), v(D, D), v(D, D)]
        + [v(T, D)] * 4
        + [v(T, 256)] * 3
        + [v(256, T), v(T, 128, t=f32), v(8, T, t=f32), v(8, T, t=f32)]
        + [v(T, 256)] * 2
        + [v(T, D)] * 2
        + [v(T, 512), v(T, 512), v(T, 256), v(T, 256)] * 3
        + [v(T, 256, t=f32)] * 2
        + [v(256, T, t=f32), v(T, 256, t=f32), v(T, 256, t=f32), v(T, 256), v(T, 256), v(3, T, 256)]
        + [v(4, 256, 512)] * 3
        + [v(ndp - 1, 4, n1, 512), v(4, n1, 512)]
        + [v(512, D)] * 3
        + [v(ndp - 1, n2, D), v(n2, D)]
        + [v(4, 3, 256, 128)] * 3
        + [v(ndp - 1, 4, 3, n1, 128), v(4, 3, n1, 128)]
        + [v(512, 256)] * 3
        + [v(ndp - 1, n2, 256), v(n2, 256)]
        + [v(4, 4, 16, 128, t=f32), v(8, 8, 128, t=f32), v(2, 8, 512, t=f32), v(8, 512, t=f32)]
        + [v(nl, 8, 512, t=f32), v(nl, 8, D, t=f32)]
        + [pltpu.SemaphoreType.DMA((N_SEM + 12 * ndp,))] * 2
        + [pltpu.SemaphoreType.DMA((32,))]
    )
    return pl.pallas_call(
        functools.partial(mega, ndp),
        out_shape=[o[0] for o in outs],
        in_specs=[hbm] * 6 + [vmem] * 6,
        out_specs=[o[1] for o in outs],
        scratch_shapes=scratch,
        name="block",
        compiler_params=pltpu.CompilerParams(
            collective_id=0, has_side_effects=True, vmem_limit_bytes=67043328
        ),
    )(*args)


def body(
    inputs, cond, w_ada, b_ada, w_qkv, b_qv, w_out, b_out, w_fc1, b_fc1, w_fc2, b_fc2, cotangent
):
    assert cond.shape[0] == 1 and inputs.shape == (T, 256)
    ndp = lax.axis_size("dp")
    act_cond = jax.nn.silu(cond).astype(bf16)
    modulation = (
        jnp.einsum("sd,dke->ske", act_cond, w_ada, preferred_element_type=f32) + b_ada[None]
    )[0]
    mod8 = jnp.concatenate([modulation, jnp.zeros((2, 256), f32)], axis=0)
    actb = jnp.broadcast_to(act_cond.astype(f32), (8, D))
    (
        result, grad_inputs, gq, go, g1, g2, gm, act_all, gmo, gbqv, gbfc1, gbout, gbfc2, gbada,
    ) = call_mega(
        ndp, inputs, cotangent, w_qkv, w_out, w_fc1, w_fc2, mod8, actb,
        b_qv, b_out[None], b_fc1[None], b_fc2[None],
    )
    grad_w_ada = jnp.einsum(
        "ld,lke->dke", act_all, gm[:, :6], precision=lax.Precision.HIGHEST,
        preferred_element_type=f32,
    )
    grad_silu = lax.psum(
        jnp.einsum(
            "ke,dke->d", gmo[:6], w_ada.astype(f32), precision=lax.Precision.HIGHEST,
            preferred_element_type=f32,
        )[None],
        "col",
    )
    grad_cond = jax.vjp(jax.nn.silu, cond)[1](grad_silu)[0]
    return (
        result,
        grad_inputs,
        grad_cond,
        grad_w_ada,
        gbada,
        gq.astype(f32),
        gbqv,
        go.astype(f32),
        gbout[0],
        g1.astype(f32),
        gbfc1[0],
        g2.reshape(2048, 256).astype(f32),
        gbfc2[0],
    )


def solution(mesh):
    return jax.shard_map(
        body,
        mesh=mesh,
        in_specs=(
            P(("dp", "row"), "col"),
            P(("dp", "row"), None),
            P(None, None, "col"),
            P(None, "col"),
            P(None, "col", "row"),
            P(None, ("row", "col")),
            P("row", "col"),
            P("col"),
            P("col", "row"),
            P(("row", "col")),
            P("row", "col"),
            P("col"),
            P(("dp", "row"), "col"),
        ),
        out_specs=(
            P(("dp", "row"), "col"),
            P(("dp", "row"), "col"),
            P(("dp", "row"), None),
            P(None, None, "col"),
            P(None, "col"),
            P(None, "col", "row"),
            P(None, ("row", "col")),
            P("row", "col"),
            P("col"),
            P("col", "row"),
            P(("row", "col")),
            P("row", "col"),
            P("col"),
        ),
        check_vma=False,
    )
```

```python
import functools

import jax
import jax.numpy as jnp
from jax import lax
from jax.experimental import pallas as pl
from jax.experimental.pallas import tpu as pltpu
from jax.sharding import PartitionSpec as P

D = 1024
HD = 64
T = 1024
EPSILON = 1e-06
bf16, f32 = jnp.bfloat16, jnp.float32
MESH = pl.DeviceIdType.MESH
NN = ((1,), (0,))
NT = ((1,), (1,))
TN = ((0,), (0,))
FACTOR = HD ** (-0.5)
LOG2E = 1.4426950408889634
TRACE = False
PLAN = (
    (97, 105, 117.5, 122.5),
    (100, 110, 121, 125.5),
    (107.5, 117.5, 125.5, 131.5),
    (112.5, 121, 131.5, 136),
    (117.5, 128.5, 138, 149),
    (122.5, 131.5, 139.5, 150),
    (128.5, 138, 147, 152),
    (136, 144, 153, 156),
    (138, 147, 155, 156),
    (142.5, 151, 159, 162),
    (147, 156, 164, 167),
    (151, 160, 168, 171),
)
GC = 0.7978845608028654
N_SEM = 256


def dot(a, b, dims):
    return lax.dot_general(a, b, (dims, ((), ())), preferred_element_type=f32)


def loop(count, step):
    def one(i, carry):
        step(i)
        return carry

    lax.fori_loop(0, count, one, 0)


def at(start, size):
    if isinstance(start, int):
        return pl.ds(start, size)
    return pl.ds(pl.multiple_of(start, size), size)


def rows_of(i, size):
    return at(i * size, size)


def mega(
    ndp,
    x_hbm,
    cot_hbm,
    wqkv,
    wout,
    wfc1,
    wfc2,
    mod,
    actb,
    bqv,
    bout,
    bfc1,
    bfc2,
    res_o,
    gin_o,
    gq_o,
    go_o,
    g1_o,
    g2_o,
    gm_o,
    act_o,
    gmo_o,
    gbqv_o,
    gbfc1_o,
    gbout_o,
    gbfc2_o,
    gbada_o,
    X,
    COT,
    N1,
    N2,
    ATT,
    WQ,
    WOUT,
    WF1,
    WF2,
    H1,
    MIX,
    H2,
    GM,
    Q,
    K,
    V,
    KT,
    LT,
    L8,
    I8,
    GA,
    ACT,
    GPRE,
    SA,
    SAR,
    YA,
    YAR,
    SC,
    SCR,
    YC,
    YCR,
    ACCA,
    DQT,
    DK,
    DV,
    QM,
    DOM,
    GQKV,
    X1S,
    X1R,
    ZS1,
    ZR1,
    ZC1,
    X2S,
    X2R,
    ZS2,
    ZR2,
    ZC2,
    XQS,
    XQR,
    ZSQ,
    ZRQ,
    ZCQ,
    XOS,
    XOR,
    ZSO,
    ZRO,
    ZCO,
    ST,
    CV,
    SBX,
    SVL,
    SVA,
    ACA,
    BQV,
    ss,
    rs,
    ls,
):
    nl = 2 * ndp
    DO = GA
    d, r, c = lax.axis_index("dp"), lax.axis_index("row"), lax.axis_index("col")
    me = d * 2 + r
    sib, yc, dg = c + 1 - 2 * (c % 2), (c + 2) % 4, 3 - c
    dev_s, dev_y, dev_g, dev_x = (d, r, sib), (d, r, yc), (d, r, dg), (d, 1 - r, c)
    q_ = 1 - r

    count = [0, 0]

    def sem(k=1):
        base = count[0]
        count[0] += k
        assert count[0] <= ss.shape[0]
        return base

    def lsem(k=1):
        base = count[1]
        count[1] += k
        assert count[1] <= ls.shape[0]
        return base

    def rc(src, dst, i, dev):
        return pltpu.make_async_remote_copy(
            src_ref=src,
            dst_ref=dst,
            send_sem=ss.at[i],
            recv_sem=rs.at[i],
            device_id=dev,
            device_id_type=MESH,
        )

    def lc(src, dst, i):
        return pltpu.make_async_copy(src, dst, ls.at[i])

    finals = []
    scope = []

    def phase(name):
        if TRACE:
            if scope:
                scope.pop().__exit__(None, None, None)
            if name:
                scope.append(jax.named_scope(name))
                scope[-1].__enter__()

    lane256 = lax.broadcasted_iota(jnp.int32, (256, 256), 1) // HD
    lane128 = lax.broadcasted_iota(jnp.int32, (128, 128), 1)

    phase("p00_start")
    cx, ccot = lc(x_hbm, X, lsem()), lc(cot_hbm, COT, lsem())
    cx.start()
    ccot.start()
    barrier = pltpu.get_barrier_semaphore()
    for dev in (dev_s, dev_y, dev_g):
        pl.semaphore_signal(barrier, inc=1, device_id=dev, device_id_type=MESH)

    def greet(o):
        other = (me + o + 1) % nl
        pl.semaphore_signal(
            barrier, inc=1, device_id=(other // 2, other % 2, c), device_id_type=MESH
        )

    loop(nl - 1, greet)
    pl.semaphore_wait(barrier, nl + 2)

    relations = ((sib, dev_s), (yc, dev_y), (dg, dev_g))

    class Weight:
        def __init__(self, src, dst):
            self.src, self.dst = src, dst
            self.a, self.x, self.l = sem(4), sem(4), lsem()
            self.z = sem(2 * (ndp - 1))

        def start(self):
            lc(self.src(c, None), self.dst(c, r, None), self.l).start()
            for rel, (to, dev) in enumerate(relations):
                z = None if rel == 0 else d
                cp = rc(self.src(to, z), self.dst(c, r, z), self.a + 1 + rel, dev)
                cp.start()
                finals.append(cp.wait_send)

        def spread(self):
            for rel in (1, 2):
                cs, dev = relations[rel]
                part = self.dst(cs, r, d)
                rc(part, part, self.a + 1 + rel, dev).wait_recv()
                base = self.z + (rel - 1) * (ndp - 1)

                def one(o):
                    rc(part, part, base + o, ((d + o + 1) % ndp, r, c)).start()

                loop(ndp - 1, one)

        def forward(self, rel):
            if rel == -1:
                self.hand(self.src(c, None), c, rel)
                return
            cs, dev = relations[rel]
            if rel == 0:
                here = self.dst(cs, r, None)
                rc(here, here, self.a + 1, dev).wait_recv()
            else:
                base = self.z + (rel - 1) * (ndp - 1)

                def one(o):
                    part = self.dst(cs, r, (d + ndp - o - 1) % ndp)
                    rc(part, part, base + o, ((d + o + 1) % ndp, r, c)).wait()

                loop(ndp - 1, one)
            self.hand(self.dst(cs, r, None), cs, rel)

        def hand(self, block, cs, rel):
            cp = rc(block, self.dst(cs, r, None), self.x + 1 + rel, dev_x)
            cp.start()
            finals.append(cp.wait_send)

        def wait_own(self):
            lc(self.src(c, None), self.dst(c, r, None), self.l).wait()

        def wait_other(self):
            for rel, cs in enumerate((c, sib, yc, dg)):
                there = self.dst(cs, q_, None)
                rc(there, there, self.x + rel, dev_x).wait_recv()

    def part(start, size, z):
        if z is None:
            return at(start, size)
        return at(start + z * (size // ndp), size // ndp)

    w_qkv = Weight(
        lambda c2, z: wqkv.at[:, part(0, 256, z), at(c2 * 128, 128)],
        lambda cs, ro, z: WQ.at[:, part(cs * 256, 256, z), at(ro * 128, 128)],
    )
    w_fc1 = Weight(
        lambda c2, z: wfc1.at[part(0, 256, z), at(c2 * 512, 512)],
        lambda cs, ro, z: WF1.at[part(cs * 256, 256, z), at(ro * 512, 512)],
    )
    w_fc2 = Weight(
        lambda c2, z: wfc2.at[part(c2 * 512, 512, z), :],
        lambda cs, ro, z: WF2.at[part(ro * 512, 512, z), at(cs * 256, 256)],
    )
    phase("p01_wsend")
    w_qkv.start()
    w_qkv.forward(-1)

    SBX[r, 0:1, :] = bfc1[...]
    SBX[r, 1:2, 0:128] = bqv[0:1, :]
    SBX[r, 1:2, 128:256] = bqv[1:2, :]
    sbx = sem()
    cp = rc(SBX.at[r], SBX.at[r], sbx, dev_x)
    cp.start()
    finals.append(cp.wait_send)

    wo, wol = sem(4), lsem(4)

    def start_wout():
        for cs in range(4):
            place = WOUT.at[at(256 * cs + 128 * r, 128), :]
            cp = rc(wout.at[at(cs * 128, 128), :], place, wo + cs, dev_x)
            cp.start()
            finals.append(cp.wait_send)
            lc(wout.at[at(cs * 128, 128), :], place, wol + cs).start()

    def wait_wout():
        for cs in range(4):
            place = WOUT.at[at(256 * cs + 128 * r, 128), :]
            lc(wout.at[at(cs * 128, 128), :], place, wol + cs).wait()
            there = WOUT.at[at(256 * cs + 128 * q_, 128), :]
            rc(there, there, wo + cs, dev_x).wait_recv()

    class ToAll:
        def __init__(self, buf):
            self.buf, self.s = buf, sem(nl - 1)

        def start(self):
            def one(o):
                other = (me + o + 1) % nl
                rc(self.buf.at[me], self.buf.at[me], self.s + o, (other // 2, other % 2, c)).start()

            loop(nl - 1, one)

        def wait(self):
            def one(o):
                other = (me + nl - o - 1) % nl
                rc(self.buf.at[other], self.buf.at[other], self.s + o, dev_x).wait()

            loop(nl - 1, one)

    class Gather:
        def __init__(self, buf):
            self.buf, self.s = buf, sem(12)
            finals.append(lambda: loop(4, self.drain))

        def reg(self, i, cs):
            return self.buf.at[rows_of(i, 256), at(cs * 256, 256)]

        def start(self, i):
            mine = self.reg(i, c)
            rc(mine, mine, self.s + i, dev_y).start()
            rc(mine, mine, self.s + 4 + i, dev_s).start()

        def forward(self, i):
            theirs = self.reg(i, yc)
            rc(theirs, theirs, self.s + i, dev_y).wait_recv()
            rc(theirs, theirs, self.s + 8 + i, dev_s).start()

        def wait(self, i):
            a, b = self.reg(i, sib), self.reg(i, dg)
            rc(a, a, self.s + 4 + i, dev_s).wait_recv()
            rc(b, b, self.s + 8 + i, dev_s).wait_recv()

        def drain(self, i):
            mine, theirs = self.reg(i, c), self.reg(i, yc)
            rc(mine, mine, self.s + i, dev_y).wait_send()
            rc(mine, mine, self.s + 4 + i, dev_s).wait_send()
            rc(theirs, theirs, self.s + 8 + i, dev_s).wait_send()

    class Scatter:
        def __init__(self, part, snd, srec, ysnd, yrec, acc):
            self.part, self.snd, self.srec = part, snd, srec
            self.ysnd, self.yrec, self.acc = ysnd, yrec, acc
            self.s = sem(8)

        def one(self, i):
            rows = rows_of(i, 256)
            self.snd[rows, 0:256] = self.part(i, dg).astype(bf16)
            self.snd[rows, 256:512] = self.part(i, sib).astype(bf16)
            rc(self.snd.at[rows], self.srec.at[rows], self.s + i, dev_s).start()

        def two(self, i):
            rows = rows_of(i, 256)
            value = self.part(i, yc)
            rc(self.snd.at[rows], self.srec.at[rows], self.s + i, dev_s).wait_recv()
            self.ysnd[rows, :] = (value + self.srec[rows, 0:256].astype(f32)).astype(bf16)
            rc(self.ysnd.at[rows], self.yrec.at[rows], self.s + 4 + i, dev_y).start()

        def three(self, i):
            rows = rows_of(i, 256)
            self.acc[rows, :] = self.part(i, c) + self.srec[rows, 256:512].astype(f32)

        def four(self, i):
            rows = rows_of(i, 256)
            rc(self.ysnd.at[rows], self.yrec.at[rows], self.s + 4 + i, dev_y).wait_recv()
            return self.acc[rows, :] + self.yrec[rows, :].astype(f32)

        def drain(self):
            def one(i):
                rows = rows_of(i, 256)
                rc(self.snd.at[rows], self.srec.at[rows], self.s + i, dev_s).wait_send()
                rc(self.ysnd.at[rows], self.yrec.at[rows], self.s + 4 + i, dev_y).wait_send()

            loop(4, one)

        def launch(self):
            loop(4, self.one)
            loop(4, self.two)
            loop(4, self.three)

    class Stats:
        def __init__(self, e):
            self.e, self.s = e, sem(3)

        def put(self, i, a, b):
            both = jnp.where(lane128 == 0, a, jnp.where(lane128 == 1, b, 0.0)).T
            ST[self.e, c, pl.ds(i, 1), :] = both[0:1, :]
            ST[self.e, c, pl.ds(8 + i, 1), :] = both[1:2, :]

        def exchange(self):
            mine = ST.at[self.e, c]
            for n, dev in enumerate((dev_s, dev_y, dev_g)):
                cp = rc(mine, mine, self.s + n, dev)
                cp.start()
                finals.append(cp.wait_send)

        def total(self):
            for n, (dev, cs) in enumerate(((dev_s, sib), (dev_y, yc), (dev_g, dg))):
                there = ST.at[self.e, cs]
                rc(there, there, self.s + n, dev).wait_recv()
            total = ST[self.e, 0] + ST[self.e, 1] + ST[self.e, 2] + ST[self.e, 3]
            return total[0:8, :], total[8:16, :]

    def column(n, i):
        half = jnp.broadcast_to(CV[n, pl.ds(i, 1), :], (128, 128)).T
        return jnp.concatenate([half, half], axis=1)

    def token_sum(value):
        return jnp.sum(value, axis=0, keepdims=True)

    def shift(k):
        return mod[3 * k - 3 : 3 * k - 2, :]

    def scale(k):
        return 1.0 + mod[3 * k - 2 : 3 * k - 1, :]

    def gate(k):
        return mod[3 * k - 1 : 3 * k, :]

    mine = at(256 * c, 256)
    SVL[...] = jnp.zeros_like(SVL)
    G_SHIFT1, G_SCALE1, G_GATE1 = (2, 0), (2, 256), (3, 0)
    G_SHIFT2, G_SCALE2, G_GATE2 = (3, 256), (4, 0), (4, 256)

    def add_to(where, value):
        row, lane = where
        SVL[row : row + 1, lane : lane + value.shape[1]] += value

    phase("p02_n1")
    ACA[me] = actb[...]
    aca = ToAll(ACA)
    st1, st2, st3, st4 = Stats(0), Stats(1), Stats(2), Stats(3)
    cx.wait()

    def n1_sums(i):
        x = X[rows_of(i, 128), :]
        st1.put(i, jnp.sum(x, axis=1, keepdims=True), jnp.sum(x * x, axis=1, keepdims=True))

    loop(8, n1_sums)
    st1.exchange()
    w_qkv.forward(0)
    ccot.wait()

    def gm_step(i):
        rows = rows_of(i, 128)
        g = COT[rows, :] * gate(2)
        add_to((6, 256), token_sum(g))
        GM[rows, mine] = g.astype(bf16)

    loop(8, gm_step)
    w_qkv.spread()
    phase("p03_n1stat")
    s1, s2 = st1.total()
    average = s1 / D
    CV[0] = average
    CV[1] = lax.rsqrt(s2 / D - average * average + EPSILON)
    ag_h1, ag_mix, ag_h2, ag_gm = Gather(H1), Gather(MIX), Gather(H2), Gather(GM)

    def n1_norm(i):
        for s in range(2):
            rows = at(i * 256 + s * 128, 128)
            normed = (X[rows, :] - column(0, 2 * i + s)) * column(1, 2 * i + s)
            N1[rows, :] = normed
            H1[rows, mine] = (normed * scale(1) + shift(1)).astype(bf16)
        ag_h1.start(i)

    phase("p04_n1norm")
    loop(4, n1_norm)
    phase("p05_wqkvfwd")
    w_fc1.start()
    w_fc2.start()
    ag_gm.start(0)
    ag_gm.start(1)
    w_qkv.forward(1)
    w_qkv.forward(2)
    start_wout()
    w_fc1.forward(-1)
    w_fc1.forward(0)
    w_fc2.forward(-1)
    w_fc2.forward(0)
    phase("p06_h1fwd")
    loop(4, ag_h1.forward)
    phase("p07_wqkvwait")
    there = SBX.at[q_]
    rc(there, there, sbx, dev_x).wait_recv()
    w_qkv.wait_own()
    w_qkv.wait_other()

    def qkv_step(i):
        ag_h1.wait(i)
        rows = rows_of(i, 256)
        h = H1[rows, :]
        qb = jnp.concatenate([SBX[0, 1:2, 0:128], SBX[1, 1:2, 0:128]], axis=1)
        vb = jnp.concatenate([SBX[0, 1:2, 128:256], SBX[1, 1:2, 128:256]], axis=1)
        Q[rows, :] = (dot(h, WQ[0], NN) + qb).astype(bf16)
        K[rows, :] = dot(h, WQ[1], NN).astype(bf16)
        V[rows, :] = (dot(h, WQ[2], NN) + vb).astype(bf16)

    phase("p08_qkv")
    loop(4, qkv_step)

    def att_step(i):
        rows = rows_of(i, 256)
        qt = Q[rows, :]
        out = jnp.zeros((256, 256), f32)
        logs = jnp.zeros((256, 128), f32)
        lane = lax.broadcasted_iota(jnp.int32, (256, 128), 1)
        for h in range(4):
            qm = jnp.where(lane256 == h, qt, jnp.zeros_like(qt))
            s = dot(qm, K[...], NT)
            m = jnp.max(s, axis=1, keepdims=True)
            p = jnp.exp2((s - m) * (FACTOR * LOG2E))
            total = jnp.sum(p, axis=1, keepdims=True)
            o = dot(p.astype(bf16), V[...], NN)
            out = jnp.where(lane256 == h, o / total, out)
            logs = jnp.where(lane == h, m * (FACTOR * LOG2E) + jnp.log2(total), logs)
        MIX[rows, mine] = out.astype(bf16)
        LT[rows, :] = logs
        ag_mix.start(i)

    w_fc1.spread()
    w_fc2.spread()
    aca.start()
    phase("p09_att")
    loop(4, att_step)
    phase("p10_fc1fwd")
    ag_gm.start(2)
    ag_gm.start(3)
    for rel in (1, 2):
        w_fc1.forward(rel)
    for rel in (1, 2):
        w_fc2.forward(rel)
    phase("p11_mixfwd")
    ag_gm.forward(0)
    ag_gm.forward(1)
    loop(4, ag_mix.forward)

    phase("p12_woutwait")
    wait_wout()

    def out_step(i):
        ag_mix.wait(i)
        rows = rows_of(i, 256)
        att = dot(MIX[rows, :], WOUT[...], NN) + bout[...]
        ATT[rows, :] = att
        X[rows, :] = X[rows, :] + gate(1) * att

    phase("p13_outproj")
    loop(4, out_step)

    def n2_sums(i):
        x = X[rows_of(i, 128), :]
        st2.put(i, jnp.sum(x, axis=1, keepdims=True), jnp.sum(x * x, axis=1, keepdims=True))

    phase("p14_n2sums")
    loop(8, n2_sums)
    st2.exchange()
    ag_gm.forward(2)
    ag_gm.forward(3)
    phase("p15_n2stat")
    s1, s2 = st2.total()
    average = s1 / D
    CV[2] = average
    CV[3] = lax.rsqrt(s2 / D - average * average + EPSILON)

    def n2_norm(i):
        for s in range(2):
            rows = at(i * 256 + s * 128, 128)
            normed = (X[rows, :] - column(2, 2 * i + s)) * column(3, 2 * i + s)
            N2[rows, :] = normed
            H2[rows, mine] = (normed * scale(2) + shift(2)).astype(bf16)
        ag_h2.start(i)

    phase("p16_n2norm")
    loop(4, n2_norm)
    phase("p19_h2fwd")
    loop(4, ag_h2.forward)
    w_fc1.wait_own()
    w_fc2.wait_own()

    def mlp_step(half, units):
        def step(i):
            rows = rows_of(i, 256)
            v = dot(H2[rows, :], WF1[:, units], NN) + SBX[half, 0:1, :]
            g = dot(GM[rows, :], WF2[units, :], NT)
            sq = v * v
            t = jnp.tanh(GC * v * (1.0 + 0.044715 * sq))
            hf = 0.5 * (1.0 + t)
            ACT[rows, units] = (v * hf).astype(bf16)
            slope = hf + (0.5 * GC) * v * (1.0 - t * t) * (1.0 + (3 * 0.044715) * sq)
            g = g * slope
            SVL[pl.ds(half, 1), :] += token_sum(g)
            GPRE[rows, units] = g.astype(bf16)

        return step

    loop(4, ag_gm.wait)
    loop(4, ag_h2.wait)
    phase("p20_mlp0")
    loop(4, mlp_step(r, at(512 * r, 512)))
    phase("p21_fcwait")
    w_fc1.wait_other()
    w_fc2.wait_other()
    phase("p21_mlp1")
    loop(4, mlp_step(q_, at(512 * q_, 512)))

    rs_h2 = Scatter(
        lambda i, b: dot(GPRE[rows_of(i, 256), :], WF1[at(b * 256, 256), :], NT),
        SA, SAR, YA, YAR, ACCA,
    )
    phase("p22_rsh2")
    rs_h2.launch()

    x1, x2, xq, xo = sem(4), sem(4), sem(3), sem()

    half = ndp // 2
    upper = d >= half
    inward = jnp.where(upper, d - 1, d + 1)
    outward = jnp.where(upper, (d + 1) % ndp, (d + ndp - 1) % ndp)
    pos = jnp.where(upper, ndp - 1 - d, d)
    dev_in, dev_out = (inward, r, c), (outward, r, c)

    class Piece:
        def __init__(self, plan, xsend, xrecv, xs, send, recv, across, regions, steps, block, place):
            self.plan = list(plan)
            self.xsend, self.xrecv, self.xs = xsend, xrecv, xs
            self.send, self.recv, self.across, self.regions = send, recv, across, regions
            self.steps, self.block, self.place = steps, block, place
            self.s, self.c, self.g, self.a, self.l = sem(), sem(), sem(len(regions)), sem(4), lsem()
            self.state = 0

        def add(self, other):
            count_, cut = self.steps

            def one(i):
                k = cut(i)
                self.send[k] = (self.send[k].astype(f32) + other[k].astype(f32)).astype(bf16)

            loop(count_, one)

        def spread(self):
            lc(self.block(c), self.place(c), self.l).start()
            if self.a is not None:
                for rel, (to, dev) in enumerate(relations):
                    rc(self.block(to), self.place(c), self.a + rel, dev).start()

        def spread_wait(self):
            lc(self.block(c), self.place(c), self.l).wait()
            if self.a is not None:
                for rel, (cs, dev) in enumerate(relations):
                    rc(self.block(cs), self.place(cs), self.a + rel, dev).wait()
            for n, region in enumerate(self.regions):
                rc(region, region, self.g + n, dev_out).start()

        def step(self):
            k = self.state
            self.state += 1
            up = rc(self.send, self.recv, self.s, dev_in)
            cross = rc(self.send, self.across, self.c, dev_in)
            if k == 0:
                rc(self.xsend, self.xrecv, self.xs, dev_x).wait()
                self.add(self.xrecv)
                for t in range(half - 1):

                    @pl.when(pos == t)
                    def _():
                        if t > 0:
                            up.wait_recv()
                            self.add(self.recv)
                        up.start()

            elif k == 1:

                @pl.when(pos == half - 1)
                def _():
                    up.wait_recv()
                    self.add(self.recv)
                    cross.start()

            elif k == 2:

                @pl.when(pos == half - 1)
                def _():
                    cross.wait()
                    self.add(self.across)
                    self.spread()

            elif k == 3:
                pl.when(pos == half - 1)(self.spread_wait)
            else:
                outs = [rc(a, a, self.g + n, dev_out) for n, a in enumerate(self.regions)]

                for t in range(half - 2, -1, -1):

                    @pl.when(pos == t)
                    def _():
                        for out in outs:
                            out.wait_recv()
                            if t > 0:
                                out.start()

                @pl.when(pos > 0)
                def _():
                    for out in outs:
                        out.wait_send()

                pl.when(pos < half - 1)(up.wait_send)

    pieces = []
    for n in range(4):
        k = (n // 2, slice(None), pl.ds(128 * (n % 2), 128), slice(None))
        pieces.append(
            Piece(
                PLAN[n],
                X1S.at[k], X1R.at[k], x1 + n, ZS1.at[k], ZR1.at[k], ZC1.at[k],
                [g1_o.at[k[2], pl.ds(512 * cs + 256 * k[0], 256)] for cs in range(4)], (4, lambda i: i),
                lambda c2, k=k: ZS1.at[k[0], c2, k[2], :],
                lambda cs, k=k: g1_o.at[k[2], at(cs * 512 + 256 * k[0], 256)],
            )
        )
    for n in range(4):
        b = pl.ds(128 * n, 128)
        pieces.append(
            Piece(
                PLAN[4 + n],
                X2S.at[b], X2R.at[b], x2 + n, ZS2.at[b], ZR2.at[b], ZC2.at[b],
                [g2_o.at[:, b, :]], (4, lambda i: (rows_of(i, 32), slice(None))),
                lambda c2, b=b: ZS2.at[b, at(256 * c2, 256)],
                lambda cs, b=b: g2_o.at[cs, b, :],
            )
        )
    piece_o = Piece(
        PLAN[8],
        XOS, XOR, xo, ZSO, ZRO, ZCO,
        [go_o], (4, lambda i: (rows_of(i, 128), slice(None))),
        lambda c2: ZSO, lambda cs: go_o,
    )
    piece_o.a = None
    pieces.append(piece_o)
    for n in range(3):
        pieces.append(
            Piece(
                PLAN[9 + n],
                XQS.at[n], XQR.at[n], xq + n, ZSQ.at[n], ZRQ.at[n], ZCQ.at[n],
                [gq_o.at[n]], (4, lambda i: i),
                lambda c2, n=n: ZSQ.at[n, c2],
                lambda cs, n=n: gq_o.at[n, :, at(128 * cs, 128)],
            )
        )

    def tick(now):
        due = sorted((p.plan[k], n, k) for n, p in enumerate(pieces) for k in range(p.state, 4) if p.plan[k] <= now)
        for _, n, k in due:
            assert pieces[n].state == k
            if now > 900:
                phase(f"p52_{n:02d}_{k}")
            pieces[n].step()

    def dw1_half(p):
        def step(i):
            h = H2[:, rows_of(i, 256)]
            X1S[p, i] = dot(h, GPRE[:, at(512 * q_ + 256 * p, 256)], TN).astype(bf16)
            ZS1[p, i] = dot(h, GPRE[:, at(512 * r + 256 * p, 256)], TN).astype(bf16)

        loop(4, step)
        for n in range(2):
            b = pl.ds(128 * n, 128)
            rc(X1S.at[p, :, b, :], X1R.at[p, :, b, :], x1 + 2 * p + n, dev_x).start()

    phase("p23_dw1")
    dw1_half(0)
    dw1_half(1)

    rs_out = Scatter(
        lambda i, b: dot(ACT[rows_of(i, 256), :], WF2[:, at(b * 256, 256)], NN),
        SC, SCR, YC, YCR, ACCA,
    )

    def dw2_step(i):
        rows = rows_of(i, 256)
        X2S[rows, :] = dot(ACT[:, at(512 * q_ + 256 * i, 256)], GM[...], TN).astype(bf16)
        for n in range(2):
            block = at(256 * i + 128 * n, 128)
            rc(X2S.at[block], X2R.at[block], x2 + 2 * i + n, dev_x).start()
        ZS2[rows, :] = dot(ACT[:, at(512 * r + 256 * i, 256)], GM[...], TN).astype(bf16)

    phase("p25_dw2")
    loop(2, dw2_step)
    tick(92)

    def b2_sums(i):
        value = rs_h2.four(i)
        ACCA[rows_of(i, 256), :] = value
        for s in range(2):
            rows = at(i * 256 + s * 128, 128)
            gh, normed = ACCA[rows, :], N2[rows, :]
            add_to(G_SHIFT2, token_sum(gh))
            hn = gh * normed
            add_to(G_SCALE2, token_sum(hn))
            st3.put(
                2 * i + s,
                jnp.sum(gh * scale(2), axis=1, keepdims=True),
                jnp.sum(hn * scale(2), axis=1, keepdims=True),
            )

    phase("p26_b2sums")
    loop(4, b2_sums)
    st3.exchange()
    phase("p27_b2stat")
    s1, s2 = st3.total()
    CV[4] = s1 / D
    CV[5] = s2 / D

    def b2_back(i):
        rows = rows_of(i, 128)
        inner = ACCA[rows, :] * scale(2) - column(4, i) - N2[rows, :] * column(5, i)
        gmid = COT[rows, :] + column(3, i) * inner
        N2[rows, :] = gmid
        ga = gmid * gate(1)
        add_to((6, 0), token_sum(ga))
        add_to(G_GATE1, token_sum(gmid * ATT[rows, :]))
        GA[rows, :] = ga.astype(bf16)

    def out_done(i):
        value = rs_out.four(i) + bfc2[...]
        rows = rows_of(i, 256)
        add_to(G_GATE2, token_sum(COT[rows, :] * value))
        X[rows, :] = X[rows, :] + gate(2) * value

    phase("p29_b2back")
    loop(8, b2_back)
    tick(97)
    rs_mix = Scatter(
        lambda i, b: dot(GA[rows_of(i, 256), :], WOUT[at(b * 256, 256), :], NT),
        SC, SCR, YC, YCR, ACCA,
    )
    phase("p30_rsmix")
    loop(4, rs_mix.one)
    loop(4, rs_mix.two)
    tick(100)
    loop(4, rs_mix.three)

    def dwo_step(i):
        rows = rows_of(i, 128)
        XOS[rows, :] = dot(MIX[:, at(256 * i + 128 * q_, 128)], GA[...], TN).astype(bf16)
        ZSO[rows, :] = dot(MIX[:, at(256 * i + 128 * r, 128)], GA[...], TN).astype(bf16)

    phase("p31_dwo")
    loop(4, dwo_step)
    rc(XOS, XOR, xo, dev_x).start()
    tick(103)

    def do_step(i):
        DO[rows_of(i, 256), :] = rs_mix.four(i).astype(bf16)

    def inner_step(i):
        rows = rows_of(i, 128)
        prod = DO[rows, :].astype(f32) * MIX[rows, mine].astype(f32)
        lane = lax.broadcasted_iota(jnp.int32, (128, 256), 1) // HD
        inner = jnp.zeros((128, 128), f32)
        for h in range(4):
            one = jnp.sum(jnp.where(lane == h, prod, 0.0), axis=1, keepdims=True)
            inner = jnp.where(lane128 == h, one, inner)
        I8[:, rows] = inner.T[0:8, :]
        L8[:, rows] = LT[rows, :].T[0:8, :]

    def kt_step(i):
        rows = rows_of(i, 256)
        KT[:, rows] = K[rows, :].astype(f32).T.astype(bf16)

    phase("p33_kt")
    loop(4, kt_step)
    BQV[...] = jnp.zeros_like(BQV)
    phase("p34_do")
    for i in range(4):
        do_step(i)
        tick(105 + 2.5 * i)
    phase("p35_inner")
    loop(8, inner_step)
    lane_all = lax.broadcasted_iota(jnp.int32, (1024, 256), 1) // HD

    def head_back(n, half, now):
        h = 2 * half + n
        QM[...] = jnp.where(lane_all == h, Q[...], jnp.zeros_like(Q[...]))
        DOM[...] = jnp.where(lane_all == h, DO[...], jnp.zeros_like(DO[...]))
        feats = at(h * HD, HD)
        lanes = at(half * 128, 128)

        def step(i, first):
            rows = rows_of(i, 512)
            p = jnp.exp2(dot(K[rows, :], QM[...], NT) * (FACTOR * LOG2E) - L8[pl.ds(h, 1), :])
            dp = dot(V[rows, :], DOM[...], NT)
            ds = (p * (dp - I8[pl.ds(h, 1), :])).astype(bf16)
            gv = dot(p.astype(bf16), DOM[:, lanes], NN)
            gk = dot(ds, QM[:, lanes], NN)
            if n == 0:
                DV[rows, lanes] = gv
                DK[rows, lanes] = gk
            else:
                DV[rows, lanes] += gv
                DK[rows, lanes] += gk
            gq = dot(KT[feats, rows], ds, NN)

            if first:
                DQT[feats, :] = gq
            else:
                DQT[feats, :] += gq

        step(0, True)
        step(1, False)
        tick(now)

    def gqkv_half(half):
        feats, lanes = at(128 * half, 128), at(128 * half, 128)

        def step(i):
            rows = rows_of(i, 256)
            gq = DQT[feats, rows].T * FACTOR
            gk, gv = DK[rows, lanes] * FACTOR, DV[rows, lanes]
            BQV[half, 0:1, :] += token_sum(gq)
            BQV[half, 1:2, :] += token_sum(gv)
            GQKV[0, rows, lanes] = gq.astype(bf16)
            GQKV[1, rows, lanes] = gk.astype(bf16)
            GQKV[2, rows, lanes] = gv.astype(bf16)

        loop(4, step)

    def dwq_half(half, out, j):
        lanes = at(128 * half, 128)

        def step(i):
            out[j, i] = dot(H1[:, rows_of(i, 256)], GQKV[j, :, lanes], TN).astype(bf16)

        loop(4, step)

    phase("p36_head0")
    head_back(0, q_, 116)
    tick(117.5)
    phase("p36_head1")
    head_back(1, q_, 119)
    gqkv_half(q_)
    phase("p37_dwq0")
    for j in range(3):
        dwq_half(q_, XQS, j)
        rc(XQS.at[j], XQR.at[j], xq + j, dev_x).start()
        tick(122.5 + 1.5 * j)
    phase("p38_head2")
    head_back(0, r, 127)
    tick(128.5)
    phase("p39_head3")
    head_back(1, r, 130)
    gqkv_half(r)
    tick(131.5)

    def part_h1(i, b):
        rows, feats = rows_of(i, 256), at(b * 256, 256)
        total = dot(GQKV[0, rows, :], WQ[0, feats, :], NT)
        total = total + dot(GQKV[1, rows, :], WQ[1, feats, :], NT)
        return total + dot(GQKV[2, rows, :], WQ[2, feats, :], NT)

    phase("p43_rsh1")
    rs_h2.drain()
    rs_h1 = Scatter(part_h1, SA, SAR, YA, YAR, ACCA)
    loop(4, rs_h1.one)
    loop(4, rs_h1.two)
    phase("p44_three")
    loop(4, rs_h1.three)
    tick(136)
    phase("p44_dwq1")
    for j in range(3):
        dwq_half(r, ZSQ, j)
        tick(138 + 1.5 * j)

    def b1_sums(i):
        value = rs_h1.four(i)
        ACCA[rows_of(i, 256), :] = value
        for s in range(2):
            rows = at(i * 256 + s * 128, 128)
            gh, normed = ACCA[rows, :], N1[rows, :]
            add_to(G_SHIFT1, token_sum(gh))
            hn = gh * normed
            add_to(G_SCALE1, token_sum(hn))
            st4.put(
                2 * i + s,
                jnp.sum(gh * scale(1), axis=1, keepdims=True),
                jnp.sum(hn * scale(1), axis=1, keepdims=True),
            )

    phase("p48_b1sums")
    for i in range(4):
        b1_sums(i)
        tick(142.5 + 1.5 * i)
    st4.exchange()
    phase("p50_b1stat")
    s1, s2 = st4.total()
    CV[6] = s1 / D
    CV[7] = s2 / D

    def b1_back(i):
        rows = rows_of(i, 128)
        inner = ACCA[rows, :] * scale(1) - column(6, i) - N1[rows, :] * column(7, i)
        N2[rows, :] = N2[rows, :] + column(1, i) * inner

    phase("p51_b1back")
    loop(8, b1_back)
    put_grad = lc(N2, gin_o, lsem())
    put_grad.start()
    finals.append(put_grad.wait)
    tick(151)
    phase("p51_rsout")
    rs_mix.drain()
    loop(4, rs_out.one)
    loop(4, rs_out.two)
    loop(4, rs_out.three)
    tick(153)
    tick(156)
    for i in range(4):
        out_done(i)
        tick(158 + 2.5 * i)
    put_result = lc(X, res_o, lsem())
    put_result.start()
    finals.append(put_result.wait)
    SVL[5:6, 0:128] = BQV[0, 0:1, :]
    SVL[5:6, 128:256] = BQV[1, 0:1, :]
    SVL[5:6, 256:384] = BQV[0, 1:2, :]
    SVL[5:6, 384:512] = BQV[1, 1:2, :]
    SVA[me] = SVL[...]
    sva = ToAll(SVA)
    sva.start()

    phase("p52_ticks")
    tick(1000)

    phase("p56_sva")
    aca.wait()
    sva.wait()
    total = jnp.zeros((8, 512), f32)
    for l in range(nl):
        one = SVA[l]
        total = total + one
        act_o[l] = ACA[l]
        for k in range(6):
            gm_o[l, k : k + 1, :] = one[2 + k // 2 : 3 + k // 2, 256 * (k % 2) : 256 * (k % 2) + 256]
        gm_o[l, 6:8, :] = jnp.zeros((2, 256), f32)
    gmo_o[...] = gm_o[me]
    first = r == 0
    for k in range(6):
        gbada_o[k : k + 1, :] = total[2 + k // 2 : 3 + k // 2, 256 * (k % 2) : 256 * (k % 2) + 256]
    gbfc1_o[...] = jnp.where(first, total[0:1, :], total[1:2, :])
    gbqv_o[0:1, :] = jnp.where(first, total[5:6, 0:128], total[5:6, 128:256])
    gbqv_o[1:2, :] = jnp.where(first, total[5:6, 256:384], total[5:6, 384:512])
    gbout_o[...] = total[6:7, 0:256]
    gbfc2_o[...] = total[6:7, 256:512]

    phase("p57_finals")
    rs_out.drain()
    rs_h1.drain()
    for one in finals:
        one()
    phase("p58_pieces")
    for n, one in enumerate(pieces):
        phase(f"p59_{n:02d}")
        one.step()
    phase("")


def call_mega(ndp, *args):
    nl = 2 * ndp
    s = jax.ShapeDtypeStruct
    vmem = pl.BlockSpec(memory_space=pltpu.VMEM)
    hbm = pl.BlockSpec(memory_space=pl.ANY)
    outs = (
        (s((T, 256), f32), hbm),
        (s((T, 256), f32), hbm),
        (s((3, 256, 512), bf16), hbm),
        (s((512, 256), bf16), hbm),
        (s((256, 2048), bf16), hbm),
        (s((4, 512, 256), bf16), hbm),
        (s((nl, 8, 256), f32), vmem),
        (s((nl, 8, 128), f32), vmem),
        (s((8, 256), f32), vmem),
        (s((2, 128), f32), vmem),
        (s((1, 512), f32), vmem),
        (s((1, 256), f32), vmem),
        (s((1, 256), f32), vmem),
        (s((6, 256), f32), vmem),
    )

    def v(*shape, t=bf16):
        return pltpu.VMEM(shape, t)

    scratch = (
        [v(T, 256, t=f32)] * 5
        + [v(3, D, 256), v(D, 256), v(D, D), v(D, D)]
        + [v(T, D)] * 4
        + [v(T, 256)] * 3
        + [v(256, T), v(T, 128, t=f32), v(8, T, t=f32), v(8, T, t=f32)]
        + [v(T, 256)]
        + [v(T, D)] * 2
        + [v(T, 512), v(T, 512), v(T, 256), v(T, 256)] * 2
        + [v(T, 256, t=f32)]
        + [v(256, T, t=f32), v(T, 256, t=f32), v(T, 256, t=f32), v(T, 256), v(T, 256), v(3, T, 256)]
        + [v(2, 4, 256, 256)] * 5
        + [v(512, D)] * 5
        + [v(3, 4, 256, 128)] * 5
        + [v(512, 256)] * 5
        + [v(4, 4, 16, 128, t=f32), v(8, 8, 128, t=f32), v(2, 8, 512, t=f32), v(8, 512, t=f32)]
        + [v(nl, 8, 512, t=f32), v(nl, 8, 128, t=f32), v(2, 8, 128, t=f32)]
        + [pltpu.SemaphoreType.DMA((N_SEM + 16 * ndp,))] * 2
        + [pltpu.SemaphoreType.DMA((40,))]
    )
    return pl.pallas_call(
        functools.partial(mega, ndp),
        out_shape=[o[0] for o in outs],
        in_specs=[hbm] * 6 + [vmem] * 6,
        out_specs=[o[1] for o in outs],
        scratch_shapes=scratch,
        name="block",
        compiler_params=pltpu.CompilerParams(
            collective_id=0, has_side_effects=True, vmem_limit_bytes=67043328
        ),
    )(*args)


def body(
    inputs, cond, w_ada, b_ada, w_qkv, b_qv, w_out, b_out, w_fc1, b_fc1, w_fc2, b_fc2, cotangent
):
    assert cond.shape[0] == 1 and inputs.shape == (T, 256)
    ndp = lax.axis_size("dp")
    act_cond = jax.nn.silu(cond).astype(bf16)
    modulation = (
        jnp.einsum("sd,dke->ske", act_cond, w_ada, preferred_element_type=f32) + b_ada[None]
    )[0]
    mod8 = jnp.concatenate([modulation, jnp.zeros((2, 256), f32)], axis=0)
    actb = act_cond.astype(f32).reshape(8, 128)
    (
        result, grad_inputs, gq, go, g1, g2, gm, act_all, gmo, gbqv, gbfc1, gbout, gbfc2, gbada,
    ) = call_mega(
        ndp, inputs, cotangent, w_qkv, w_out, w_fc1, w_fc2, mod8, actb,
        b_qv, b_out[None], b_fc1[None], b_fc2[None],
    )
    grad_w_ada = jnp.einsum(
        "ld,lke->dke", act_all.reshape(-1, D), gm[:, :6], precision=lax.Precision.HIGHEST,
        preferred_element_type=f32,
    )
    grad_silu = lax.psum(
        jnp.einsum(
            "ke,dke->d", gmo[:6], w_ada.astype(f32), precision=lax.Precision.HIGHEST,
            preferred_element_type=f32,
        )[None],
        "col",
    )
    grad_cond = jax.vjp(jax.nn.silu, cond)[1](grad_silu)[0]
    return (
        result,
        grad_inputs,
        grad_cond,
        grad_w_ada,
        gbada,
        gq.astype(f32),
        gbqv,
        go.astype(f32),
        gbout[0],
        g1.astype(f32),
        gbfc1[0],
        g2.reshape(2048, 256).astype(f32),
        gbfc2[0],
    )


def solution(mesh):
    return jax.shard_map(
        body,
        mesh=mesh,
        in_specs=(
            P(("dp", "row"), "col"),
            P(("dp", "row"), None),
            P(None, None, "col"),
            P(None, "col"),
            P(None, "col", "row"),
            P(None, ("row", "col")),
            P("row", "col"),
            P("col"),
            P("col", "row"),
            P(("row", "col")),
            P("row", "col"),
            P("col"),
            P(("dp", "row"), "col"),
        ),
        out_specs=(
            P(("dp", "row"), "col"),
            P(("dp", "row"), "col"),
            P(("dp", "row"), None),
            P(None, None, "col"),
            P(None, "col"),
            P(None, "col", "row"),
            P(None, ("row", "col")),
            P("row", "col"),
            P("col"),
            P("col", "row"),
            P(("row", "col")),
            P("row", "col"),
            P("col"),
        ),
        check_vma=False,
    )
```

```python
import functools

import jax
import jax.numpy as jnp
from jax import lax
from jax.experimental import pallas as pl
from jax.experimental.pallas import tpu as pltpu
from jax.sharding import PartitionSpec as P

D = 1024
HD = 64
T = 1024
EPSILON = 1e-06
bf16, f32 = jnp.bfloat16, jnp.float32
MESH = pl.DeviceIdType.MESH
NN = ((1,), (0,))
NT = ((1,), (1,))
TN = ((0,), (0,))
FACTOR = HD ** (-0.5)
LOG2E = 1.4426950408889634
TRACE = False
PLAN = (
    (97, 105, 117.5, 122.5),
    (100, 110, 121, 125.5),
    (107.5, 117.5, 125.5, 131.5),
    (112.5, 121, 131.5, 136),
    (117.5, 128.5, 138, 149),
    (122.5, 131.5, 139.5, 150),
    (128.5, 138, 147, 152),
    (136, 144, 153, 156),
    (138, 147, 155, 156),
    (142.5, 151, 159, 162),
    (147, 156, 164, 167),
    (151, 160, 168, 171),
)
GC = 0.7978845608028654
N_SEM = 256


def dot(a, b, dims):
    return lax.dot_general(a, b, (dims, ((), ())), preferred_element_type=f32)


def loop(count, step):
    def one(i, carry):
        step(i)
        return carry

    lax.fori_loop(0, count, one, 0)


def at(start, size):
    if isinstance(start, int):
        return pl.ds(start, size)
    return pl.ds(pl.multiple_of(start, size), size)


def rows_of(i, size):
    return at(i * size, size)


def mega(
    ndp,
    x_hbm,
    cot_hbm,
    wqkv,
    wout,
    wfc1,
    wfc2,
    mod,
    actb,
    bqv,
    bout,
    bfc1,
    bfc2,
    res_o,
    gin_o,
    gq_o,
    go_o,
    g1_o,
    g2_o,
    gm_o,
    act_o,
    gmo_o,
    gbqv_o,
    gbfc1_o,
    gbout_o,
    gbfc2_o,
    gbada_o,
    X,
    COT,
    N1,
    N2,
    ATT,
    WQ,
    WOUT,
    WF1,
    WF2,
    H1,
    MIX,
    H2,
    GM,
    Q,
    K,
    V,
    KT,
    LT,
    L8,
    I8,
    GA,
    ACT,
    GPRE,
    SA,
    SAR,
    YA,
    YAR,
    SC,
    SCR,
    YC,
    YCR,
    ACCA,
    DQT,
    DK,
    DV,
    QM,
    DOM,
    GQKV,
    X1S,
    X1R,
    ZS1,
    ZR1,
    ZC1,
    X2S,
    X2R,
    ZS2,
    ZR2,
    ZC2,
    XQS,
    XQR,
    ZSQ,
    ZRQ,
    ZCQ,
    XOS,
    XOR,
    ZSO,
    ZRO,
    ZCO,
    ST,
    CV,
    SBX,
    SVL,
    SVA,
    ACA,
    BQV,
    ss,
    rs,
    ls,
):
    nl = 2 * ndp
    DO = GA
    d, r, c = lax.axis_index("dp"), lax.axis_index("row"), lax.axis_index("col")
    me = d * 2 + r
    sib, yc, dg = c + 1 - 2 * (c % 2), (c + 2) % 4, 3 - c
    dev_s, dev_y, dev_g, dev_x = (d, r, sib), (d, r, yc), (d, r, dg), (d, 1 - r, c)
    q_ = 1 - r

    count = [0, 0]

    def sem(k=1):
        base = count[0]
        count[0] += k
        assert count[0] <= ss.shape[0]
        return base

    def lsem(k=1):
        base = count[1]
        count[1] += k
        assert count[1] <= ls.shape[0]
        return base

    def rc(src, dst, i, dev):
        return pltpu.make_async_remote_copy(
            src_ref=src,
            dst_ref=dst,
            send_sem=ss.at[i],
            recv_sem=rs.at[i],
            device_id=dev,
            device_id_type=MESH,
        )

    def lc(src, dst, i):
        return pltpu.make_async_copy(src, dst, ls.at[i])

    finals = []
    scope = []

    def phase(name):
        if TRACE:
            if scope:
                scope.pop().__exit__(None, None, None)
            if name:
                scope.append(jax.named_scope(name))
                scope[-1].__enter__()

    lane256 = lax.broadcasted_iota(jnp.int32, (256, 256), 1) // HD
    lane128 = lax.broadcasted_iota(jnp.int32, (128, 128), 1)

    phase("p00_start")
    cx, ccot = lc(x_hbm, X, lsem()), lc(cot_hbm, COT, lsem())
    cx.start()
    ccot.start()
    barrier = pltpu.get_barrier_semaphore()
    for dev in (dev_s, dev_y, dev_g):
        pl.semaphore_signal(barrier, inc=1, device_id=dev, device_id_type=MESH)

    def greet(o):
        other = (me + o + 1) % nl
        pl.semaphore_signal(
            barrier, inc=1, device_id=(other // 2, other % 2, c), device_id_type=MESH
        )

    loop(nl - 1, greet)
    pl.semaphore_wait(barrier, nl + 2)

    relations = ((sib, dev_s), (yc, dev_y), (dg, dev_g))

    class Weight:
        def __init__(self, src, dst):
            self.src, self.dst = src, dst
            self.a, self.x, self.l = sem(4), sem(4), lsem()
            self.z = sem(2 * (ndp - 1))

        def start(self):
            lc(self.src(c, None), self.dst(c, r, None), self.l).start()
            for rel, (to, dev) in enumerate(relations):
                z = None if rel == 0 else d
                cp = rc(self.src(to, z), self.dst(c, r, z), self.a + 1 + rel, dev)
                cp.start()
                finals.append(cp.wait_send)

        def spread(self):
            for rel in (1, 2):
                cs, dev = relations[rel]
                part = self.dst(cs, r, d)
                rc(part, part, self.a + 1 + rel, dev).wait_recv()
                base = self.z + (rel - 1) * (ndp - 1)

                def one(o):
                    rc(part, part, base + o, ((d + o + 1) % ndp, r, c)).start()

                loop(ndp - 1, one)

        def forward(self, rel):
            if rel == -1:
                self.hand(self.src(c, None), c, rel)
                return
            cs, dev = relations[rel]
            if rel == 0:
                here = self.dst(cs, r, None)
                rc(here, here, self.a + 1, dev).wait_recv()
            else:
                base = self.z + (rel - 1) * (ndp - 1)

                def one(o):
                    part = self.dst(cs, r, (d + ndp - o - 1) % ndp)
                    rc(part, part, base + o, ((d + o + 1) % ndp, r, c)).wait()

                loop(ndp - 1, one)
            self.hand(self.dst(cs, r, None), cs, rel)

        def hand(self, block, cs, rel):
            cp = rc(block, self.dst(cs, r, None), self.x + 1 + rel, dev_x)
            cp.start()
            finals.append(cp.wait_send)

        def wait_own(self):
            lc(self.src(c, None), self.dst(c, r, None), self.l).wait()

        def wait_other(self):
            for rel, cs in enumerate((c, sib, yc, dg)):
                there = self.dst(cs, q_, None)
                rc(there, there, self.x + rel, dev_x).wait_recv()

    def part(start, size, z):
        if z is None:
            return at(start, size)
        return at(start + z * (size // ndp), size // ndp)

    w_qkv = Weight(
        lambda c2, z: wqkv.at[:, part(0, 256, z), at(c2 * 128, 128)],
        lambda cs, ro, z: WQ.at[:, part(cs * 256, 256, z), at(ro * 128, 128)],
    )
    w_fc1 = Weight(
        lambda c2, z: wfc1.at[part(0, 256, z), at(c2 * 512, 512)],
        lambda cs, ro, z: WF1.at[part(cs * 256, 256, z), at(ro * 512, 512)],
    )
    w_fc2 = Weight(
        lambda c2, z: wfc2.at[part(c2 * 512, 512, z), :],
        lambda cs, ro, z: WF2.at[part(ro * 512, 512, z), at(cs * 256, 256)],
    )
    phase("p01_wsend")
    w_qkv.start()
    w_qkv.forward(-1)

    SBX[r, 0:1, :] = bfc1[...]
    SBX[r, 1:2, 0:128] = bqv[0:1, :]
    SBX[r, 1:2, 128:256] = bqv[1:2, :]
    sbx = sem()
    cp = rc(SBX.at[r], SBX.at[r], sbx, dev_x)
    cp.start()
    finals.append(cp.wait_send)

    wo, wol = sem(4), lsem(4)

    def start_wout():
        for cs in range(4):
            place = WOUT.at[at(256 * cs + 128 * r, 128), :]
            cp = rc(wout.at[at(cs * 128, 128), :], place, wo + cs, dev_x)
            cp.start()
            finals.append(cp.wait_send)
            lc(wout.at[at(cs * 128, 128), :], place, wol + cs).start()

    def wait_wout():
        for cs in range(4):
            place = WOUT.at[at(256 * cs + 128 * r, 128), :]
            lc(wout.at[at(cs * 128, 128), :], place, wol + cs).wait()
            there = WOUT.at[at(256 * cs + 128 * q_, 128), :]
            rc(there, there, wo + cs, dev_x).wait_recv()

    class ToAll:
        def __init__(self, buf):
            self.buf, self.s = buf, sem(nl - 1)

        def start(self):
            def one(o):
                other = (me + o + 1) % nl
                rc(self.buf.at[me], self.buf.at[me], self.s + o, (other // 2, other % 2, c)).start()

            loop(nl - 1, one)

        def wait(self):
            def one(o):
                other = (me + nl - o - 1) % nl
                rc(self.buf.at[other], self.buf.at[other], self.s + o, dev_x).wait()

            loop(nl - 1, one)

    class Gather:
        def __init__(self, buf):
            self.buf, self.s = buf, sem(12)
            finals.append(lambda: loop(4, self.drain))

        def reg(self, i, cs):
            return self.buf.at[rows_of(i, 256), at(cs * 256, 256)]

        def start(self, i):
            mine = self.reg(i, c)
            rc(mine, mine, self.s + i, dev_y).start()
            rc(mine, mine, self.s + 4 + i, dev_s).start()

        def forward(self, i):
            theirs = self.reg(i, yc)
            rc(theirs, theirs, self.s + i, dev_y).wait_recv()
            rc(theirs, theirs, self.s + 8 + i, dev_s).start()

        def wait(self, i):
            a, b = self.reg(i, sib), self.reg(i, dg)
            rc(a, a, self.s + 4 + i, dev_s).wait_recv()
            rc(b, b, self.s + 8 + i, dev_s).wait_recv()

        def drain(self, i):
            mine, theirs = self.reg(i, c), self.reg(i, yc)
            rc(mine, mine, self.s + i, dev_y).wait_send()
            rc(mine, mine, self.s + 4 + i, dev_s).wait_send()
            rc(theirs, theirs, self.s + 8 + i, dev_s).wait_send()

    class Scatter:
        def __init__(self, part, snd, srec, ysnd, yrec, acc):
            self.part, self.snd, self.srec = part, snd, srec
            self.ysnd, self.yrec, self.acc = ysnd, yrec, acc
            self.s = sem(8)

        def one(self, i):
            rows = rows_of(i, 256)
            self.snd[rows, 0:256] = self.part(i, dg).astype(bf16)
            self.snd[rows, 256:512] = self.part(i, sib).astype(bf16)
            rc(self.snd.at[rows], self.srec.at[rows], self.s + i, dev_s).start()

        def two(self, i):
            rows = rows_of(i, 256)
            value = self.part(i, yc)
            rc(self.snd.at[rows], self.srec.at[rows], self.s + i, dev_s).wait_recv()
            self.ysnd[rows, :] = (value + self.srec[rows, 0:256].astype(f32)).astype(bf16)
            rc(self.ysnd.at[rows], self.yrec.at[rows], self.s + 4 + i, dev_y).start()

        def three(self, i):
            rows = rows_of(i, 256)
            self.acc[rows, :] = self.part(i, c) + self.srec[rows, 256:512].astype(f32)

        def four(self, i):
            rows = rows_of(i, 256)
            rc(self.ysnd.at[rows], self.yrec.at[rows], self.s + 4 + i, dev_y).wait_recv()
            return self.acc[rows, :] + self.yrec[rows, :].astype(f32)

        def drain(self):
            def one(i):
                rows = rows_of(i, 256)
                rc(self.snd.at[rows], self.srec.at[rows], self.s + i, dev_s).wait_send()
                rc(self.ysnd.at[rows], self.yrec.at[rows], self.s + 4 + i, dev_y).wait_send()

            loop(4, one)

        def launch(self):
            loop(4, self.one)
            loop(4, self.two)
            loop(4, self.three)

    class Stats:
        def __init__(self, e):
            self.e, self.s = e, sem(3)

        def put(self, i, a, b):
            both = jnp.where(lane128 == 0, a, jnp.where(lane128 == 1, b, 0.0)).T
            ST[self.e, c, pl.ds(i, 1), :] = both[0:1, :]
            ST[self.e, c, pl.ds(8 + i, 1), :] = both[1:2, :]

        def exchange(self):
            mine = ST.at[self.e, c]
            for n, dev in enumerate((dev_s, dev_y, dev_g)):
                cp = rc(mine, mine, self.s + n, dev)
                cp.start()
                finals.append(cp.wait_send)

        def total(self):
            for n, (dev, cs) in enumerate(((dev_s, sib), (dev_y, yc), (dev_g, dg))):
                there = ST.at[self.e, cs]
                rc(there, there, self.s + n, dev).wait_recv()
            total = ST[self.e, 0] + ST[self.e, 1] + ST[self.e, 2] + ST[self.e, 3]
            return total[0:8, :], total[8:16, :]

    def column(n, i):
        half = jnp.broadcast_to(CV[n, pl.ds(i, 1), :], (128, 128)).T
        return jnp.concatenate([half, half], axis=1)

    def token_sum(value):
        return jnp.sum(value, axis=0, keepdims=True)

    def shift(k):
        return mod[3 * k - 3 : 3 * k - 2, :]

    def scale(k):
        return 1.0 + mod[3 * k - 2 : 3 * k - 1, :]

    def gate(k):
        return mod[3 * k - 1 : 3 * k, :]

    mine = at(256 * c, 256)
    SVL[...] = jnp.zeros_like(SVL)
    G_SHIFT1, G_SCALE1, G_GATE1 = (2, 0), (2, 256), (3, 0)
    G_SHIFT2, G_SCALE2, G_GATE2 = (3, 256), (4, 0), (4, 256)

    def add_to(where, value):
        row, lane = where
        SVL[row : row + 1, lane : lane + value.shape[1]] += value

    phase("p02_n1")
    ACA[me] = actb[...]
    aca = ToAll(ACA)
    st1, st2, st3, st4 = Stats(0), Stats(1), Stats(2), Stats(3)
    cx.wait()

    def n1_sums(i):
        x = X[rows_of(i, 128), :]
        st1.put(i, jnp.sum(x, axis=1, keepdims=True), jnp.sum(x * x, axis=1, keepdims=True))

    loop(8, n1_sums)
    st1.exchange()
    w_qkv.forward(0)
    ccot.wait()

    def gm_step(i):
        rows = rows_of(i, 128)
        g = COT[rows, :] * gate(2)
        add_to((6, 256), token_sum(g))
        GM[rows, mine] = g.astype(bf16)

    loop(8, gm_step)
    w_qkv.spread()
    phase("p03_n1stat")
    s1, s2 = st1.total()
    average = s1 / D
    CV[0] = average
    CV[1] = lax.rsqrt(s2 / D - average * average + EPSILON)
    ag_h1, ag_mix, ag_h2, ag_gm = Gather(H1), Gather(MIX), Gather(H2), Gather(GM)

    def n1_norm(i):
        for s in range(2):
            rows = at(i * 256 + s * 128, 128)
            normed = (X[rows, :] - column(0, 2 * i + s)) * column(1, 2 * i + s)
            N1[rows, :] = normed
            H1[rows, mine] = (normed * scale(1) + shift(1)).astype(bf16)
        ag_h1.start(i)

    phase("p04_n1norm")
    loop(4, n1_norm)
    phase("p05_wqkvfwd")
    w_fc1.start()
    w_fc2.start()
    ag_gm.start(0)
    ag_gm.start(1)
    w_qkv.forward(1)
    w_qkv.forward(2)
    start_wout()
    w_fc1.forward(-1)
    w_fc1.forward(0)
    w_fc2.forward(-1)
    w_fc2.forward(0)
    phase("p06_h1fwd")
    loop(4, ag_h1.forward)
    phase("p07_wqkvwait")
    there = SBX.at[q_]
    rc(there, there, sbx, dev_x).wait_recv()
    w_qkv.wait_own()
    w_qkv.wait_other()

    def qkv_step(i):
        ag_h1.wait(i)
        rows = rows_of(i, 256)
        h = H1[rows, :]
        qb = jnp.concatenate([SBX[0, 1:2, 0:128], SBX[1, 1:2, 0:128]], axis=1)
        vb = jnp.concatenate([SBX[0, 1:2, 128:256], SBX[1, 1:2, 128:256]], axis=1)
        Q[rows, :] = (dot(h, WQ[0], NN) + qb).astype(bf16)
        K[rows, :] = dot(h, WQ[1], NN).astype(bf16)
        V[rows, :] = (dot(h, WQ[2], NN) + vb).astype(bf16)

    phase("p08_qkv")
    loop(4, qkv_step)

    def att_step(i):
        rows = rows_of(i, 256)
        qt = Q[rows, :]
        out = jnp.zeros((256, 256), f32)
        logs = jnp.zeros((256, 128), f32)
        lane = lax.broadcasted_iota(jnp.int32, (256, 128), 1)
        for h in range(4):
            qm = jnp.where(lane256 == h, qt, jnp.zeros_like(qt))
            s = dot(qm, K[...], NT)
            m = jnp.max(s, axis=1, keepdims=True)
            p = jnp.exp2((s - m) * (FACTOR * LOG2E))
            total = jnp.sum(p, axis=1, keepdims=True)
            o = dot(p.astype(bf16), V[...], NN)
            out = jnp.where(lane256 == h, o / total, out)
            logs = jnp.where(lane == h, m * (FACTOR * LOG2E) + jnp.log2(total), logs)
        MIX[rows, mine] = out.astype(bf16)
        LT[rows, :] = logs
        ag_mix.start(i)

    w_fc1.spread()
    w_fc2.spread()
    aca.start()
    phase("p09_att")
    loop(4, att_step)
    phase("p10_fc1fwd")
    ag_gm.start(2)
    ag_gm.start(3)
    for rel in (1, 2):
        w_fc1.forward(rel)
    for rel in (1, 2):
        w_fc2.forward(rel)
    phase("p11_mixfwd")
    ag_gm.forward(0)
    ag_gm.forward(1)
    loop(4, ag_mix.forward)

    phase("p12_woutwait")
    wait_wout()

    def out_step(i):
        ag_mix.wait(i)
        rows = rows_of(i, 256)
        att = dot(MIX[rows, :], WOUT[...], NN) + bout[...]
        ATT[rows, :] = att
        X[rows, :] = X[rows, :] + gate(1) * att

    phase("p13_outproj")
    loop(4, out_step)

    def n2_sums(i):
        x = X[rows_of(i, 128), :]
        st2.put(i, jnp.sum(x, axis=1, keepdims=True), jnp.sum(x * x, axis=1, keepdims=True))

    phase("p14_n2sums")
    loop(8, n2_sums)
    st2.exchange()
    ag_gm.forward(2)
    ag_gm.forward(3)
    phase("p15_n2stat")
    s1, s2 = st2.total()
    average = s1 / D
    CV[2] = average
    CV[3] = lax.rsqrt(s2 / D - average * average + EPSILON)

    def n2_norm(i):
        for s in range(2):
            rows = at(i * 256 + s * 128, 128)
            normed = (X[rows, :] - column(2, 2 * i + s)) * column(3, 2 * i + s)
            N2[rows, :] = normed
            H2[rows, mine] = (normed * scale(2) + shift(2)).astype(bf16)
        ag_h2.start(i)

    phase("p16_n2norm")
    loop(4, n2_norm)
    phase("p19_h2fwd")
    loop(4, ag_h2.forward)
    w_fc1.wait_own()
    w_fc2.wait_own()

    def mlp_step(half, units):
        def step(i):
            rows = rows_of(i, 256)
            v = dot(H2[rows, :], WF1[:, units], NN) + SBX[half, 0:1, :]
            g = dot(GM[rows, :], WF2[units, :], NT)
            sq = v * v
            t = jnp.tanh(GC * v * (1.0 + 0.044715 * sq))
            hf = 0.5 * (1.0 + t)
            ACT[rows, units] = (v * hf).astype(bf16)
            slope = hf + (0.5 * GC) * v * (1.0 - t * t) * (1.0 + (3 * 0.044715) * sq)
            g = g * slope
            SVL[pl.ds(half, 1), :] += token_sum(g)
            GPRE[rows, units] = g.astype(bf16)

        return step

    loop(4, ag_gm.wait)
    loop(4, ag_h2.wait)
    phase("p20_mlp0")
    loop(4, mlp_step(r, at(512 * r, 512)))
    phase("p21_fcwait")
    w_fc1.wait_other()
    w_fc2.wait_other()
    phase("p21_mlp1")
    loop(4, mlp_step(q_, at(512 * q_, 512)))

    rs_h2 = Scatter(
        lambda i, b: dot(GPRE[rows_of(i, 256), :], WF1[at(b * 256, 256), :], NT),
        SA, SAR, YA, YAR, ACCA,
    )
    phase("p22_rsh2")
    rs_h2.launch()

    x1, x2, xq, xo = sem(4), sem(4), sem(3), sem()

    half = ndp // 2
    upper = d >= half
    inward = jnp.where(upper, d - 1, d + 1)
    outward = jnp.where(upper, (d + 1) % ndp, (d + ndp - 1) % ndp)
    pos = jnp.where(upper, ndp - 1 - d, d)
    dev_in, dev_out = (inward, r, c), (outward, r, c)

    class Piece:
        def __init__(self, plan, xsend, xrecv, xs, send, recv, across, regions, steps, block, place):
            self.plan = list(plan)
            self.xsend, self.xrecv, self.xs = xsend, xrecv, xs
            self.send, self.recv, self.across, self.regions = send, recv, across, regions
            self.steps, self.block, self.place = steps, block, place
            self.s, self.c, self.g, self.a, self.l = sem(), sem(), sem(len(regions)), sem(4), lsem()
            self.state = 0

        def add(self, other):
            count_, cut = self.steps

            def one(i):
                k = cut(i)
                self.send[k] = (self.send[k].astype(f32) + other[k].astype(f32)).astype(bf16)

            loop(count_, one)

        def spread(self):
            lc(self.block(c), self.place(c), self.l).start()
            if self.a is not None:
                for rel, (to, dev) in enumerate(relations):
                    rc(self.block(to), self.place(c), self.a + rel, dev).start()

        def spread_wait(self):
            lc(self.block(c), self.place(c), self.l).wait()
            if self.a is not None:
                for rel, (cs, dev) in enumerate(relations):
                    rc(self.block(cs), self.place(cs), self.a + rel, dev).wait()
            for n, region in enumerate(self.regions):
                rc(region, region, self.g + n, dev_out).start()

        def step(self):
            k = self.state
            self.state += 1
            up = rc(self.send, self.recv, self.s, dev_in)
            cross = rc(self.send, self.across, self.c, dev_in)
            if k == 0:
                rc(self.xsend, self.xrecv, self.xs, dev_x).wait()
                self.add(self.xrecv)
                for t in range(half - 1):

                    @pl.when(pos == t)
                    def _():
                        if t > 0:
                            up.wait_recv()
                            self.add(self.recv)
                        up.start()

            elif k == 1:

                @pl.when(pos == half - 1)
                def _():
                    up.wait_recv()
                    self.add(self.recv)
                    cross.start()

            elif k == 2:

                @pl.when(pos == half - 1)
                def _():
                    cross.wait()
                    self.add(self.across)
                    self.spread()

            elif k == 3:
                pl.when(pos == half - 1)(self.spread_wait)
            else:
                outs = [rc(a, a, self.g + n, dev_out) for n, a in enumerate(self.regions)]

                for t in range(half - 2, -1, -1):

                    @pl.when(pos == t)
                    def _():
                        for out in outs:
                            out.wait_recv()
                            if t > 0:
                                out.start()

                @pl.when(pos > 0)
                def _():
                    for out in outs:
                        out.wait_send()

                pl.when(pos < half - 1)(up.wait_send)

    pieces = []
    for n in range(4):
        k = (n // 2, slice(None), pl.ds(128 * (n % 2), 128), slice(None))
        pieces.append(
            Piece(
                PLAN[n],
                X1S.at[k], X1R.at[k], x1 + n, ZS1.at[k], ZR1.at[k], ZC1.at[k],
                [g1_o.at[k[2], pl.ds(512 * cs + 256 * k[0], 256)] for cs in range(4)], (4, lambda i: i),
                lambda c2, k=k: ZS1.at[k[0], c2, k[2], :],
                lambda cs, k=k: g1_o.at[k[2], at(cs * 512 + 256 * k[0], 256)],
            )
        )
    for n in range(4):
        b = pl.ds(128 * n, 128)
        pieces.append(
            Piece(
                PLAN[4 + n],
                X2S.at[b], X2R.at[b], x2 + n, ZS2.at[b], ZR2.at[b], ZC2.at[b],
                [g2_o.at[:, b, :]], (4, lambda i: (rows_of(i, 32), slice(None))),
                lambda c2, b=b: ZS2.at[b, at(256 * c2, 256)],
                lambda cs, b=b: g2_o.at[cs, b, :],
            )
        )
    piece_o = Piece(
        PLAN[8],
        XOS, XOR, xo, ZSO, ZRO, ZCO,
        [go_o], (4, lambda i: (rows_of(i, 128), slice(None))),
        lambda c2: ZSO, lambda cs: go_o,
    )
    piece_o.a = None
    pieces.append(piece_o)
    for n in range(3):
        pieces.append(
            Piece(
                PLAN[9 + n],
                XQS.at[n], XQR.at[n], xq + n, ZSQ.at[n], ZRQ.at[n], ZCQ.at[n],
                [gq_o.at[n]], (4, lambda i: i),
                lambda c2, n=n: ZSQ.at[n, c2],
                lambda cs, n=n: gq_o.at[n, :, at(128 * cs, 128)],
            )
        )

    def tick(now):
        due = sorted((p.plan[k], n, k) for n, p in enumerate(pieces) for k in range(p.state, 4) if p.plan[k] <= now)
        for _, n, k in due:
            assert pieces[n].state == k
            if now > 900:
                phase(f"p52_{n:02d}_{k}")
            pieces[n].step()

    def dw1_half(p):
        def step(i):
            h = H2[:, rows_of(i, 256)]
            X1S[p, i] = dot(h, GPRE[:, at(512 * q_ + 256 * p, 256)], TN).astype(bf16)
            ZS1[p, i] = dot(h, GPRE[:, at(512 * r + 256 * p, 256)], TN).astype(bf16)

        loop(4, step)
        for n in range(2):
            b = pl.ds(128 * n, 128)
            rc(X1S.at[p, :, b, :], X1R.at[p, :, b, :], x1 + 2 * p + n, dev_x).start()

    phase("p23_dw1")
    dw1_half(0)
    dw1_half(1)

    rs_out = Scatter(
        lambda i, b: dot(ACT[rows_of(i, 256), :], WF2[:, at(b * 256, 256)], NN),
        SC, SCR, YC, YCR, ACCA,
    )

    def dw2_step(i):
        rows = rows_of(i, 256)
        X2S[rows, :] = dot(ACT[:, at(512 * q_ + 256 * i, 256)], GM[...], TN).astype(bf16)
        for n in range(2):
            block = at(256 * i + 128 * n, 128)
            rc(X2S.at[block], X2R.at[block], x2 + 2 * i + n, dev_x).start()
        ZS2[rows, :] = dot(ACT[:, at(512 * r + 256 * i, 256)], GM[...], TN).astype(bf16)

    phase("p25_dw2")
    loop(2, dw2_step)
    tick(92)

    def b2_sums(i):
        value = rs_h2.four(i)
        ACCA[rows_of(i, 256), :] = value
        for s in range(2):
            rows = at(i * 256 + s * 128, 128)
            gh, normed = ACCA[rows, :], N2[rows, :]
            add_to(G_SHIFT2, token_sum(gh))
            hn = gh * normed
            add_to(G_SCALE2, token_sum(hn))
            st3.put(
                2 * i + s,
                jnp.sum(gh * scale(2), axis=1, keepdims=True),
                jnp.sum(hn * scale(2), axis=1, keepdims=True),
            )

    phase("p26_b2sums")
    loop(4, b2_sums)
    st3.exchange()
    phase("p27_b2stat")
    s1, s2 = st3.total()
    CV[4] = s1 / D
    CV[5] = s2 / D

    def b2_back(i):
        rows = rows_of(i, 128)
        inner = ACCA[rows, :] * scale(2) - column(4, i) - N2[rows, :] * column(5, i)
        gmid = COT[rows, :] + column(3, i) * inner
        N2[rows, :] = gmid
        ga = gmid * gate(1)
        add_to((6, 0), token_sum(ga))
        add_to(G_GATE1, token_sum(gmid * ATT[rows, :]))
        GA[rows, :] = ga.astype(bf16)

    def out_done(i):
        value = rs_out.four(i) + bfc2[...]
        rows = rows_of(i, 256)
        add_to(G_GATE2, token_sum(COT[rows, :] * value))
        X[rows, :] = X[rows, :] + gate(2) * value

    phase("p29_b2back")
    loop(8, b2_back)
    tick(97)
    rs_mix = Scatter(
        lambda i, b: dot(GA[rows_of(i, 256), :], WOUT[at(b * 256, 256), :], NT),
        SC, SCR, YC, YCR, ACCA,
    )
    phase("p30_rsmix")
    loop(4, rs_mix.one)
    loop(4, rs_mix.two)
    tick(100)
    loop(4, rs_mix.three)

    def dwo_step(i):
        rows = rows_of(i, 128)
        XOS[rows, :] = dot(MIX[:, at(256 * i + 128 * q_, 128)], GA[...], TN).astype(bf16)
        ZSO[rows, :] = dot(MIX[:, at(256 * i + 128 * r, 128)], GA[...], TN).astype(bf16)

    phase("p31_dwo")
    loop(4, dwo_step)
    rc(XOS, XOR, xo, dev_x).start()
    tick(103)

    def do_step(i):
        DO[rows_of(i, 256), :] = rs_mix.four(i).astype(bf16)

    def inner_step(i):
        rows = rows_of(i, 128)
        prod = DO[rows, :].astype(f32) * MIX[rows, mine].astype(f32)
        lane = lax.broadcasted_iota(jnp.int32, (128, 256), 1) // HD
        inner = jnp.zeros((128, 128), f32)
        for h in range(4):
            one = jnp.sum(jnp.where(lane == h, prod, 0.0), axis=1, keepdims=True)
            inner = jnp.where(lane128 == h, one, inner)
        I8[:, rows] = inner.T[0:8, :]
        L8[:, rows] = LT[rows, :].T[0:8, :]

    def kt_step(i):
        rows = rows_of(i, 256)
        KT[:, rows] = K[rows, :].astype(f32).T.astype(bf16)

    phase("p33_kt")
    loop(4, kt_step)
    BQV[...] = jnp.zeros_like(BQV)
    phase("p34_do")
    for i in range(4):
        do_step(i)
        tick(105 + 2.5 * i)
    phase("p35_inner")
    loop(8, inner_step)
    lane_all = lax.broadcasted_iota(jnp.int32, (1024, 256), 1) // HD

    def head_back(n, half, now):
        h = 2 * half + n
        QM[...] = jnp.where(lane_all == h, Q[...], jnp.zeros_like(Q[...]))
        DOM[...] = jnp.where(lane_all == h, DO[...], jnp.zeros_like(DO[...]))
        feats = at(h * HD, HD)
        lanes = at(half * 128, 128)

        def step(i, first):
            rows = rows_of(i, 512)
            p = jnp.exp2(dot(K[rows, :], QM[...], NT) * (FACTOR * LOG2E) - L8[pl.ds(h, 1), :])
            dp = dot(V[rows, :], DOM[...], NT)
            ds = (p * (dp - I8[pl.ds(h, 1), :])).astype(bf16)
            gv = dot(p.astype(bf16), DOM[:, lanes], NN)
            gk = dot(ds, QM[:, lanes], NN)
            if n == 0:
                DV[rows, lanes] = gv
                DK[rows, lanes] = gk
            else:
                DV[rows, lanes] += gv
                DK[rows, lanes] += gk
            gq = dot(KT[feats, rows], ds, NN)

            if first:
                DQT[feats, :] = gq
            else:
                DQT[feats, :] += gq

        step(0, True)
        step(1, False)
        tick(now)

    def gqkv_half(half):
        feats, lanes = at(128 * half, 128), at(128 * half, 128)

        def step(i):
            rows = rows_of(i, 256)
            gq = DQT[feats, rows].T * FACTOR
            gk, gv = DK[rows, lanes] * FACTOR, DV[rows, lanes]
            BQV[half, 0:1, :] += token_sum(gq)
            BQV[half, 1:2, :] += token_sum(gv)
            GQKV[0, rows, lanes] = gq.astype(bf16)
            GQKV[1, rows, lanes] = gk.astype(bf16)
            GQKV[2, rows, lanes] = gv.astype(bf16)

        loop(4, step)

    def dwq_half(half, out, j):
        lanes = at(128 * half, 128)

        def step(i):
            out[j, i] = dot(H1[:, rows_of(i, 256)], GQKV[j, :, lanes], TN).astype(bf16)

        loop(4, step)

    phase("p36_head0")
    head_back(0, q_, 116)
    tick(117.5)
    phase("p36_head1")
    head_back(1, q_, 119)
    gqkv_half(q_)
    phase("p37_dwq0")
    for j in range(3):
        dwq_half(q_, XQS, j)
        rc(XQS.at[j], XQR.at[j], xq + j, dev_x).start()
        tick(122.5 + 1.5 * j)
    phase("p38_head2")
    head_back(0, r, 127)
    tick(128.5)
    phase("p39_head3")
    head_back(1, r, 130)
    gqkv_half(r)
    tick(131.5)

    def part_h1(i, b):
        rows, feats = rows_of(i, 256), at(b * 256, 256)
        total = dot(GQKV[0, rows, :], WQ[0, feats, :], NT)
        total = total + dot(GQKV[1, rows, :], WQ[1, feats, :], NT)
        return total + dot(GQKV[2, rows, :], WQ[2, feats, :], NT)

    phase("p43_rsh1")
    rs_h2.drain()
    rs_h1 = Scatter(part_h1, SA, SAR, YA, YAR, ACCA)
    loop(4, rs_h1.one)
    loop(4, rs_h1.two)
    phase("p44_three")
    loop(4, rs_h1.three)
    tick(136)
    phase("p44_dwq1")
    for j in range(3):
        dwq_half(r, ZSQ, j)
        tick(138 + 1.5 * j)

    def b1_sums(i):
        value = rs_h1.four(i)
        ACCA[rows_of(i, 256), :] = value
        for s in range(2):
            rows = at(i * 256 + s * 128, 128)
            gh, normed = ACCA[rows, :], N1[rows, :]
            add_to(G_SHIFT1, token_sum(gh))
            hn = gh * normed
            add_to(G_SCALE1, token_sum(hn))
            st4.put(
                2 * i + s,
                jnp.sum(gh * scale(1), axis=1, keepdims=True),
                jnp.sum(hn * scale(1), axis=1, keepdims=True),
            )

    phase("p48_b1sums")
    for i in range(4):
        b1_sums(i)
        tick(142.5 + 1.5 * i)
    st4.exchange()
    phase("p50_b1stat")
    s1, s2 = st4.total()
    CV[6] = s1 / D
    CV[7] = s2 / D

    def b1_back(i):
        rows = rows_of(i, 128)
        inner = ACCA[rows, :] * scale(1) - column(6, i) - N1[rows, :] * column(7, i)
        N2[rows, :] = N2[rows, :] + column(1, i) * inner

    phase("p51_b1back")
    loop(8, b1_back)
    put_grad = lc(N2, gin_o, lsem())
    put_grad.start()
    finals.append(put_grad.wait)
    tick(151)
    phase("p51_rsout")
    rs_mix.drain()
    loop(4, rs_out.one)
    loop(4, rs_out.two)
    loop(4, rs_out.three)
    tick(153)
    tick(156)
    for i in range(4):
        out_done(i)
        tick(158 + 2.5 * i)
    put_result = lc(X, res_o, lsem())
    put_result.start()
    finals.append(put_result.wait)
    SVL[5:6, 0:128] = BQV[0, 0:1, :]
    SVL[5:6, 128:256] = BQV[1, 0:1, :]
    SVL[5:6, 256:384] = BQV[0, 1:2, :]
    SVL[5:6, 384:512] = BQV[1, 1:2, :]
    SVA[me] = SVL[...]
    sva = ToAll(SVA)
    sva.start()

    phase("p52_ticks")
    tick(1000)

    phase("p56_sva")
    aca.wait()
    sva.wait()
    total = jnp.zeros((8, 512), f32)
    for l in range(nl):
        one = SVA[l]
        total = total + one
        act_o[l] = ACA[l]
        for k in range(6):
            gm_o[l, k : k + 1, :] = one[2 + k // 2 : 3 + k // 2, 256 * (k % 2) : 256 * (k % 2) + 256]
        gm_o[l, 6:8, :] = jnp.zeros((2, 256), f32)
    gmo_o[...] = gm_o[me]
    first = r == 0
    for k in range(6):
        gbada_o[k : k + 1, :] = total[2 + k // 2 : 3 + k // 2, 256 * (k % 2) : 256 * (k % 2) + 256]
    gbfc1_o[...] = jnp.where(first, total[0:1, :], total[1:2, :])
    gbqv_o[0:1, :] = jnp.where(first, total[5:6, 0:128], total[5:6, 128:256])
    gbqv_o[1:2, :] = jnp.where(first, total[5:6, 256:384], total[5:6, 384:512])
    gbout_o[...] = total[6:7, 0:256]
    gbfc2_o[...] = total[6:7, 256:512]

    phase("p57_finals")
    rs_out.drain()
    rs_h1.drain()
    for one in finals:
        one()
    phase("p58_pieces")
    for n, one in enumerate(pieces):
        phase(f"p59_{n:02d}")
        one.step()
    phase("")


def call_mega(ndp, *args):
    nl = 2 * ndp
    s = jax.ShapeDtypeStruct
    vmem = pl.BlockSpec(memory_space=pltpu.VMEM)
    hbm = pl.BlockSpec(memory_space=pl.ANY)
    outs = (
        (s((T, 256), f32), hbm),
        (s((T, 256), f32), hbm),
        (s((3, 256, 512), bf16), hbm),
        (s((512, 256), bf16), hbm),
        (s((256, 2048), bf16), hbm),
        (s((4, 512, 256), bf16), hbm),
        (s((nl, 8, 256), f32), vmem),
        (s((nl, 8, 128), f32), vmem),
        (s((8, 256), f32), vmem),
        (s((2, 128), f32), vmem),
        (s((1, 512), f32), vmem),
        (s((1, 256), f32), vmem),
        (s((1, 256), f32), vmem),
        (s((6, 256), f32), vmem),
    )

    def v(*shape, t=bf16):
        return pltpu.VMEM(shape, t)

    scratch = (
        [v(T, 256, t=f32)] * 5
        + [v(3, D, 256), v(D, 256), v(D, D), v(D, D)]
        + [v(T, D)] * 4
        + [v(T, 256)] * 3
        + [v(256, T), v(T, 128, t=f32), v(8, T, t=f32), v(8, T, t=f32)]
        + [v(T, 256)]
        + [v(T, D)] * 2
        + [v(T, 512), v(T, 512), v(T, 256), v(T, 256)] * 2
        + [v(T, 256, t=f32)]
        + [v(256, T, t=f32), v(T, 256, t=f32), v(T, 256, t=f32), v(T, 256), v(T, 256), v(3, T, 256)]
        + [v(2, 4, 256, 256)] * 5
        + [v(512, D)] * 5
        + [v(3, 4, 256, 128)] * 5
        + [v(512, 256)] * 5
        + [v(4, 4, 16, 128, t=f32), v(8, 8, 128, t=f32), v(2, 8, 512, t=f32), v(8, 512, t=f32)]
        + [v(nl, 8, 512, t=f32), v(nl, 8, 128, t=f32), v(2, 8, 128, t=f32)]
        + [pltpu.SemaphoreType.DMA((N_SEM + 16 * ndp,))] * 2
        + [pltpu.SemaphoreType.DMA((40,))]
    )
    return pl.pallas_call(
        functools.partial(mega, ndp),
        out_shape=[o[0] for o in outs],
        in_specs=[hbm] * 6 + [vmem] * 6,
        out_specs=[o[1] for o in outs],
        scratch_shapes=scratch,
        name="block",
        compiler_params=pltpu.CompilerParams(
            collective_id=0, has_side_effects=True, vmem_limit_bytes=67043328
        ),
    )(*args)


def body(
    inputs, cond, w_ada, b_ada, w_qkv, b_qv, w_out, b_out, w_fc1, b_fc1, w_fc2, b_fc2, cotangent
):
    assert cond.shape[0] == 1 and inputs.shape == (T, 256)
    ndp = lax.axis_size("dp")
    act_cond = jax.nn.silu(cond).astype(bf16)
    modulation = (
        jnp.einsum("sd,dke->ske", act_cond, w_ada, preferred_element_type=f32) + b_ada[None]
    )[0]
    mod8 = jnp.concatenate([modulation, jnp.zeros((2, 256), f32)], axis=0)
    actb = act_cond.astype(f32).reshape(8, 128)
    (
        result, grad_inputs, gq, go, g1, g2, gm, act_all, gmo, gbqv, gbfc1, gbout, gbfc2, gbada,
    ) = call_mega(
        ndp, inputs, cotangent, w_qkv, w_out, w_fc1, w_fc2, mod8, actb,
        b_qv, b_out[None], b_fc1[None], b_fc2[None],
    )
    parts = []
    rest = gm[:, :6]
    for _ in range(3):
        parts.append(lax.reduce_precision(rest, 8, 7))
        rest = rest - parts[-1]
    cut = jnp.concatenate(parts, axis=0).astype(bf16)
    act_low = jnp.concatenate([act_all.reshape(-1, D)] * 3, axis=0).astype(bf16)
    grad_w_ada = jnp.einsum("ld,lke->dke", act_low, cut, preferred_element_type=f32)
    parts = []
    rest = gmo[:6]
    for _ in range(3):
        parts.append(lax.reduce_precision(rest, 8, 7))
        rest = rest - parts[-1]
    own = jnp.stack(parts).astype(bf16)
    grad_silu = lax.psum(
        jnp.sum(
            jnp.einsum("pke,dke->pd", own, w_ada, preferred_element_type=f32),
            axis=0,
            keepdims=True,
        ),
        "col",
    )
    grad_cond = jax.vjp(jax.nn.silu, cond)[1](grad_silu)[0]
    return (
        result,
        grad_inputs,
        grad_cond,
        grad_w_ada,
        gbada,
        gq.astype(f32),
        gbqv,
        go.astype(f32),
        gbout[0],
        g1.astype(f32),
        gbfc1[0],
        g2.reshape(2048, 256).astype(f32),
        gbfc2[0],
    )


def solution(mesh):
    return jax.shard_map(
        body,
        mesh=mesh,
        in_specs=(
            P(("dp", "row"), "col"),
            P(("dp", "row"), None),
            P(None, None, "col"),
            P(None, "col"),
            P(None, "col", "row"),
            P(None, ("row", "col")),
            P("row", "col"),
            P("col"),
            P("col", "row"),
            P(("row", "col")),
            P("row", "col"),
            P("col"),
            P(("dp", "row"), "col"),
        ),
        out_specs=(
            P(("dp", "row"), "col"),
            P(("dp", "row"), "col"),
            P(("dp", "row"), None),
            P(None, None, "col"),
            P(None, "col"),
            P(None, "col", "row"),
            P(None, ("row", "col")),
            P("row", "col"),
            P("col"),
            P("col", "row"),
            P(("row", "col")),
            P("row", "col"),
            P("col"),
        ),
        check_vma=False,
    )
```

```python
import functools

import jax
import jax.numpy as jnp
from jax import lax
from jax.experimental import pallas as pl
from jax.experimental.pallas import tpu as pltpu
from jax.sharding import PartitionSpec as P

D = 1024
HD = 64
T = 1024
EPSILON = 1e-06
bf16, f32 = jnp.bfloat16, jnp.float32
MESH = pl.DeviceIdType.MESH
NN = ((1,), (0,))
NT = ((1,), (1,))
TN = ((0,), (0,))
FACTOR = HD ** (-0.5)
LOG2E = 1.4426950408889634
TRACE = False
PLAN = (
    (97, 105, 117.5, 122.5),
    (100, 110, 121, 125.5),
    (107.5, 117.5, 125.5, 131.5),
    (112.5, 121, 131.5, 136),
    (117.5, 128.5, 148, 152),
    (122.5, 131.5, 148, 153),
    (128.5, 138, 148, 154),
    (136, 144, 153, 157),
    (138, 147, 155, 156),
    (142.5, 151, 159, 162),
    (147, 156, 164, 167),
    (151, 160, 168, 171),
)
GC = 0.7978845608028654
N_SEM = 256


def dot(a, b, dims):
    return lax.dot_general(a, b, (dims, ((), ())), preferred_element_type=f32)


def loop(count, step):
    def one(i, carry):
        step(i)
        return carry

    lax.fori_loop(0, count, one, 0)


def at(start, size):
    if isinstance(start, int):
        return pl.ds(start, size)
    return pl.ds(pl.multiple_of(start, size), size)


def rows_of(i, size):
    return at(i * size, size)


def mega(
    ndp,
    x_hbm,
    cot_hbm,
    wqkv,
    wout,
    wfc1,
    wfc2,
    mod,
    actb,
    bqv,
    bout,
    bfc1,
    bfc2,
    res_o,
    gin_o,
    gq_o,
    go_o,
    g1_o,
    g2_o,
    gm_o,
    act_o,
    gmo_o,
    gbqv_o,
    gbfc1_o,
    gbout_o,
    gbfc2_o,
    gbada_o,
    X,
    COT,
    N1,
    N2,
    ATT,
    WQ,
    WOUT,
    WF1,
    WF2,
    H1,
    MIX,
    H2,
    GM,
    Q,
    K,
    V,
    KT,
    LT,
    L8,
    I8,
    GA,
    ACT,
    GPRE,
    SA,
    SAR,
    YA,
    YAR,
    SC,
    SCR,
    YC,
    YCR,
    ACCA,
    DQT,
    DK,
    DV,
    QM,
    DOM,
    GQKV,
    X1S,
    X1R,
    ZS1,
    ZR1,
    ZC1,
    X2S,
    X2R,
    ZS2,
    ZR2,
    ZC2,
    XQS,
    XQR,
    ZSQ,
    ZRQ,
    ZCQ,
    XOS,
    XOR,
    ZSO,
    ZRO,
    ZCO,
    ST,
    CV,
    SBX,
    SVL,
    SVA,
    ACA,
    BQV,
    ss,
    rs,
    ls,
):
    nl = 2 * ndp
    DO = GA
    d, r, c = lax.axis_index("dp"), lax.axis_index("row"), lax.axis_index("col")
    me = d * 2 + r
    sib, yc, dg = c + 1 - 2 * (c % 2), (c + 2) % 4, 3 - c
    dev_s, dev_y, dev_g, dev_x = (d, r, sib), (d, r, yc), (d, r, dg), (d, 1 - r, c)
    q_ = 1 - r

    count = [0, 0]

    def sem(k=1):
        base = count[0]
        count[0] += k
        assert count[0] <= ss.shape[0]
        return base

    def lsem(k=1):
        base = count[1]
        count[1] += k
        assert count[1] <= ls.shape[0]
        return base

    def rc(src, dst, i, dev):
        return pltpu.make_async_remote_copy(
            src_ref=src,
            dst_ref=dst,
            send_sem=ss.at[i],
            recv_sem=rs.at[i],
            device_id=dev,
            device_id_type=MESH,
        )

    def lc(src, dst, i):
        return pltpu.make_async_copy(src, dst, ls.at[i])

    finals = []
    scope = []

    def phase(name):
        if TRACE:
            if scope:
                scope.pop().__exit__(None, None, None)
            if name:
                scope.append(jax.named_scope(name))
                scope[-1].__enter__()

    lane256 = lax.broadcasted_iota(jnp.int32, (256, 256), 1) // HD
    lane128 = lax.broadcasted_iota(jnp.int32, (128, 128), 1)

    phase("p00_start")
    cx, ccot = lc(x_hbm, X, lsem()), lc(cot_hbm, COT, lsem())
    cx.start()
    ccot.start()
    barrier = pltpu.get_barrier_semaphore()
    for dev in (dev_s, dev_y, dev_g):
        pl.semaphore_signal(barrier, inc=1, device_id=dev, device_id_type=MESH)

    def greet(o):
        other = (me + o + 1) % nl
        pl.semaphore_signal(
            barrier, inc=1, device_id=(other // 2, other % 2, c), device_id_type=MESH
        )

    loop(nl - 1, greet)
    pl.semaphore_wait(barrier, nl + 2)

    relations = ((sib, dev_s), (yc, dev_y), (dg, dev_g))

    class Weight:
        def __init__(self, src, dst):
            self.src, self.dst = src, dst
            self.a, self.x, self.l = sem(4), sem(4), lsem()
            self.z = sem(2 * (ndp - 1))

        def start(self):
            lc(self.src(c, None), self.dst(c, r, None), self.l).start()
            for rel, (to, dev) in enumerate(relations):
                z = None if rel == 0 else d
                cp = rc(self.src(to, z), self.dst(c, r, z), self.a + 1 + rel, dev)
                cp.start()
                finals.append(cp.wait_send)

        def spread(self):
            for rel in (1, 2):
                cs, dev = relations[rel]
                part = self.dst(cs, r, d)
                rc(part, part, self.a + 1 + rel, dev).wait_recv()
                base = self.z + (rel - 1) * (ndp - 1)

                def one(o):
                    rc(part, part, base + o, ((d + o + 1) % ndp, r, c)).start()

                loop(ndp - 1, one)

        def forward(self, rel):
            if rel == -1:
                self.hand(self.src(c, None), c, rel)
                return
            cs, dev = relations[rel]
            if rel == 0:
                here = self.dst(cs, r, None)
                rc(here, here, self.a + 1, dev).wait_recv()
            else:
                base = self.z + (rel - 1) * (ndp - 1)

                def one(o):
                    part = self.dst(cs, r, (d + ndp - o - 1) % ndp)
                    rc(part, part, base + o, ((d + o + 1) % ndp, r, c)).wait()

                loop(ndp - 1, one)
            self.hand(self.dst(cs, r, None), cs, rel)

        def hand(self, block, cs, rel):
            cp = rc(block, self.dst(cs, r, None), self.x + 1 + rel, dev_x)
            cp.start()
            finals.append(cp.wait_send)

        def wait_own(self):
            lc(self.src(c, None), self.dst(c, r, None), self.l).wait()

        def wait_other(self):
            for rel, cs in enumerate((c, sib, yc, dg)):
                there = self.dst(cs, q_, None)
                rc(there, there, self.x + rel, dev_x).wait_recv()

    def part(start, size, z):
        if z is None:
            return at(start, size)
        return at(start + z * (size // ndp), size // ndp)

    w_qkv = Weight(
        lambda c2, z: wqkv.at[:, part(0, 256, z), at(c2 * 128, 128)],
        lambda cs, ro, z: WQ.at[:, part(cs * 256, 256, z), at(ro * 128, 128)],
    )
    w_fc1 = Weight(
        lambda c2, z: wfc1.at[part(0, 256, z), at(c2 * 512, 512)],
        lambda cs, ro, z: WF1.at[part(cs * 256, 256, z), at(ro * 512, 512)],
    )
    w_fc2 = Weight(
        lambda c2, z: wfc2.at[part(c2 * 512, 512, z), :],
        lambda cs, ro, z: WF2.at[part(ro * 512, 512, z), at(cs * 256, 256)],
    )
    phase("p01_wsend")
    w_qkv.start()
    w_qkv.forward(-1)

    SBX[r, 0:1, :] = bfc1[...]
    SBX[r, 1:2, 0:128] = bqv[0:1, :]
    SBX[r, 1:2, 128:256] = bqv[1:2, :]
    sbx = sem()
    cp = rc(SBX.at[r], SBX.at[r], sbx, dev_x)
    cp.start()
    finals.append(cp.wait_send)

    wo, wol = sem(4), lsem(4)

    def start_wout():
        for cs in range(4):
            place = WOUT.at[at(256 * cs + 128 * r, 128), :]
            cp = rc(wout.at[at(cs * 128, 128), :], place, wo + cs, dev_x)
            cp.start()
            finals.append(cp.wait_send)
            lc(wout.at[at(cs * 128, 128), :], place, wol + cs).start()

    def wait_wout():
        for cs in range(4):
            place = WOUT.at[at(256 * cs + 128 * r, 128), :]
            lc(wout.at[at(cs * 128, 128), :], place, wol + cs).wait()
            there = WOUT.at[at(256 * cs + 128 * q_, 128), :]
            rc(there, there, wo + cs, dev_x).wait_recv()

    class ToAll:
        def __init__(self, buf):
            self.buf, self.s = buf, sem(nl - 1)

        def start(self):
            def one(o):
                other = (me + o + 1) % nl
                rc(self.buf.at[me], self.buf.at[me], self.s + o, (other // 2, other % 2, c)).start()

            loop(nl - 1, one)

        def wait(self):
            def one(o):
                other = (me + nl - o - 1) % nl
                rc(self.buf.at[other], self.buf.at[other], self.s + o, dev_x).wait()

            loop(nl - 1, one)

    class Gather:
        def __init__(self, buf):
            self.buf, self.s = buf, sem(12)
            finals.append(lambda: loop(4, self.drain))

        def reg(self, i, cs):
            return self.buf.at[rows_of(i, 256), at(cs * 256, 256)]

        def start(self, i):
            mine = self.reg(i, c)
            rc(mine, mine, self.s + i, dev_y).start()
            rc(mine, mine, self.s + 4 + i, dev_s).start()

        def forward(self, i):
            theirs = self.reg(i, yc)
            rc(theirs, theirs, self.s + i, dev_y).wait_recv()
            rc(theirs, theirs, self.s + 8 + i, dev_s).start()

        def wait(self, i):
            a, b = self.reg(i, sib), self.reg(i, dg)
            rc(a, a, self.s + 4 + i, dev_s).wait_recv()
            rc(b, b, self.s + 8 + i, dev_s).wait_recv()

        def drain(self, i):
            mine, theirs = self.reg(i, c), self.reg(i, yc)
            rc(mine, mine, self.s + i, dev_y).wait_send()
            rc(mine, mine, self.s + 4 + i, dev_s).wait_send()
            rc(theirs, theirs, self.s + 8 + i, dev_s).wait_send()

    class Scatter:
        def __init__(self, part, snd, srec, ysnd, yrec, acc):
            self.part, self.snd, self.srec = part, snd, srec
            self.ysnd, self.yrec, self.acc = ysnd, yrec, acc
            self.s = sem(8)

        def one(self, i):
            rows = rows_of(i, 256)
            self.snd[rows, 0:256] = self.part(i, dg).astype(bf16)
            self.snd[rows, 256:512] = self.part(i, sib).astype(bf16)
            rc(self.snd.at[rows], self.srec.at[rows], self.s + i, dev_s).start()

        def two(self, i):
            rows = rows_of(i, 256)
            value = self.part(i, yc)
            rc(self.snd.at[rows], self.srec.at[rows], self.s + i, dev_s).wait_recv()
            self.ysnd[rows, :] = (value + self.srec[rows, 0:256].astype(f32)).astype(bf16)
            rc(self.ysnd.at[rows], self.yrec.at[rows], self.s + 4 + i, dev_y).start()

        def three(self, i):
            rows = rows_of(i, 256)
            self.acc[rows, :] = self.part(i, c) + self.srec[rows, 256:512].astype(f32)

        def four(self, i):
            rows = rows_of(i, 256)
            rc(self.ysnd.at[rows], self.yrec.at[rows], self.s + 4 + i, dev_y).wait_recv()
            return self.acc[rows, :] + self.yrec[rows, :].astype(f32)

        def drain(self):
            def one(i):
                rows = rows_of(i, 256)
                rc(self.snd.at[rows], self.srec.at[rows], self.s + i, dev_s).wait_send()
                rc(self.ysnd.at[rows], self.yrec.at[rows], self.s + 4 + i, dev_y).wait_send()

            loop(4, one)

        def launch(self):
            loop(4, self.one)
            loop(4, self.two)
            loop(4, self.three)

    class Stats:
        def __init__(self, e):
            self.e, self.s = e, sem(3)

        def put(self, i, a, b):
            both = jnp.where(lane128 == 0, a, jnp.where(lane128 == 1, b, 0.0)).T
            ST[self.e, c, pl.ds(i, 1), :] = both[0:1, :]
            ST[self.e, c, pl.ds(8 + i, 1), :] = both[1:2, :]

        def exchange(self):
            mine = ST.at[self.e, c]
            for n, dev in enumerate((dev_s, dev_y, dev_g)):
                cp = rc(mine, mine, self.s + n, dev)
                cp.start()
                finals.append(cp.wait_send)

        def total(self):
            for n, (dev, cs) in enumerate(((dev_s, sib), (dev_y, yc), (dev_g, dg))):
                there = ST.at[self.e, cs]
                rc(there, there, self.s + n, dev).wait_recv()
            total = ST[self.e, 0] + ST[self.e, 1] + ST[self.e, 2] + ST[self.e, 3]
            return total[0:8, :], total[8:16, :]

    def column(n, i):
        half = jnp.broadcast_to(CV[n, pl.ds(i, 1), :], (128, 128)).T
        return jnp.concatenate([half, half], axis=1)

    def token_sum(value):
        return jnp.sum(value, axis=0, keepdims=True)

    def shift(k):
        return mod[3 * k - 3 : 3 * k - 2, :]

    def scale(k):
        return 1.0 + mod[3 * k - 2 : 3 * k - 1, :]

    def gate(k):
        return mod[3 * k - 1 : 3 * k, :]

    mine = at(256 * c, 256)
    SVL[...] = jnp.zeros_like(SVL)
    G_SHIFT1, G_SCALE1, G_GATE1 = (2, 0), (2, 256), (3, 0)
    G_SHIFT2, G_SCALE2, G_GATE2 = (3, 256), (4, 0), (4, 256)

    def add_to(where, value):
        row, lane = where
        SVL[row : row + 1, lane : lane + value.shape[1]] += value

    phase("p02_n1")
    ACA[me] = actb[...]
    aca = ToAll(ACA)
    st1, st2, st3, st4 = Stats(0), Stats(1), Stats(2), Stats(3)
    cx.wait()

    def n1_sums(i):
        x = X[rows_of(i, 128), :]
        st1.put(i, jnp.sum(x, axis=1, keepdims=True), jnp.sum(x * x, axis=1, keepdims=True))

    loop(8, n1_sums)
    st1.exchange()
    w_qkv.forward(0)
    ccot.wait()

    def gm_step(i):
        rows = rows_of(i, 128)
        g = COT[rows, :] * gate(2)
        add_to((6, 256), token_sum(g))
        GM[rows, mine] = g.astype(bf16)

    loop(8, gm_step)
    w_qkv.spread()
    phase("p03_n1stat")
    s1, s2 = st1.total()
    average = s1 / D
    CV[0] = average
    CV[1] = lax.rsqrt(s2 / D - average * average + EPSILON)
    ag_h1, ag_mix, ag_h2, ag_gm = Gather(H1), Gather(MIX), Gather(H2), Gather(GM)

    def n1_norm(i):
        for s in range(2):
            rows = at(i * 256 + s * 128, 128)
            normed = (X[rows, :] - column(0, 2 * i + s)) * column(1, 2 * i + s)
            N1[rows, :] = normed
            H1[rows, mine] = (normed * scale(1) + shift(1)).astype(bf16)
        ag_h1.start(i)

    phase("p04_n1norm")
    loop(4, n1_norm)
    phase("p05_wqkvfwd")
    w_fc1.start()
    w_fc2.start()
    ag_gm.start(0)
    ag_gm.start(1)
    w_qkv.forward(1)
    w_qkv.forward(2)
    start_wout()
    w_fc1.forward(-1)
    w_fc1.forward(0)
    w_fc2.forward(-1)
    w_fc2.forward(0)
    phase("p06_h1fwd")
    loop(4, ag_h1.forward)
    phase("p07_wqkvwait")
    there = SBX.at[q_]
    rc(there, there, sbx, dev_x).wait_recv()
    w_qkv.wait_own()
    w_qkv.wait_other()

    def qkv_step(i):
        ag_h1.wait(i)
        rows = rows_of(i, 256)
        h = H1[rows, :]
        qb = jnp.concatenate([SBX[0, 1:2, 0:128], SBX[1, 1:2, 0:128]], axis=1)
        vb = jnp.concatenate([SBX[0, 1:2, 128:256], SBX[1, 1:2, 128:256]], axis=1)
        Q[rows, :] = (dot(h, WQ[0], NN) + qb).astype(bf16)
        K[rows, :] = dot(h, WQ[1], NN).astype(bf16)
        V[rows, :] = (dot(h, WQ[2], NN) + vb).astype(bf16)

    phase("p08_qkv")
    loop(4, qkv_step)

    def att_step(i):
        rows = rows_of(i, 256)
        qt = Q[rows, :]
        out = jnp.zeros((256, 256), f32)
        logs = jnp.zeros((256, 128), f32)
        lane = lax.broadcasted_iota(jnp.int32, (256, 128), 1)
        for h in range(4):
            qm = jnp.where(lane256 == h, qt, jnp.zeros_like(qt))
            s = dot(qm, K[...], NT)
            m = jnp.max(s, axis=1, keepdims=True)
            p = jnp.exp2((s - m) * (FACTOR * LOG2E))
            total = jnp.sum(p, axis=1, keepdims=True)
            o = dot(p.astype(bf16), V[...], NN)
            out = jnp.where(lane256 == h, o / total, out)
            logs = jnp.where(lane == h, m * (FACTOR * LOG2E) + jnp.log2(total), logs)
        MIX[rows, mine] = out.astype(bf16)
        LT[rows, :] = logs
        ag_mix.start(i)

    w_fc1.spread()
    w_fc2.spread()
    aca.start()
    phase("p09_att")
    loop(4, att_step)
    phase("p10_fc1fwd")
    ag_gm.start(2)
    ag_gm.start(3)
    for rel in (1, 2):
        w_fc1.forward(rel)
    for rel in (1, 2):
        w_fc2.forward(rel)
    phase("p11_mixfwd")
    ag_gm.forward(0)
    ag_gm.forward(1)
    loop(4, ag_mix.forward)

    phase("p12_woutwait")
    wait_wout()

    def out_step(i):
        ag_mix.wait(i)
        rows = rows_of(i, 256)
        att = dot(MIX[rows, :], WOUT[...], NN) + bout[...]
        ATT[rows, :] = att
        X[rows, :] = X[rows, :] + gate(1) * att

    phase("p13_outproj")
    loop(4, out_step)

    def n2_sums(i):
        x = X[rows_of(i, 128), :]
        st2.put(i, jnp.sum(x, axis=1, keepdims=True), jnp.sum(x * x, axis=1, keepdims=True))

    phase("p14_n2sums")
    loop(8, n2_sums)
    st2.exchange()
    ag_gm.forward(2)
    ag_gm.forward(3)
    phase("p15_n2stat")
    s1, s2 = st2.total()
    average = s1 / D
    CV[2] = average
    CV[3] = lax.rsqrt(s2 / D - average * average + EPSILON)

    def n2_norm(i):
        for s in range(2):
            rows = at(i * 256 + s * 128, 128)
            normed = (X[rows, :] - column(2, 2 * i + s)) * column(3, 2 * i + s)
            N2[rows, :] = normed
            H2[rows, mine] = (normed * scale(2) + shift(2)).astype(bf16)
        ag_h2.start(i)

    phase("p16_n2norm")
    loop(4, n2_norm)
    phase("p19_h2fwd")
    loop(4, ag_h2.forward)
    w_fc1.wait_own()
    w_fc2.wait_own()

    def mlp_step(half, units):
        def step(i):
            rows = rows_of(i, 256)
            v = dot(H2[rows, :], WF1[:, units], NN) + SBX[half, 0:1, :]
            g = dot(GM[rows, :], WF2[units, :], NT)
            sq = v * v
            t = jnp.tanh(GC * v * (1.0 + 0.044715 * sq))
            hf = 0.5 * (1.0 + t)
            ACT[rows, units] = (v * hf).astype(bf16)
            slope = hf + (0.5 * GC) * v * (1.0 - t * t) * (1.0 + (3 * 0.044715) * sq)
            g = g * slope
            SVL[pl.ds(half, 1), :] += token_sum(g)
            GPRE[rows, units] = g.astype(bf16)

        return step

    loop(4, ag_gm.wait)
    loop(4, ag_h2.wait)
    phase("p20_mlp0")
    loop(4, mlp_step(r, at(512 * r, 512)))
    phase("p21_fcwait")
    w_fc1.wait_other()
    w_fc2.wait_other()
    phase("p21_mlp1")
    loop(4, mlp_step(q_, at(512 * q_, 512)))

    rs_h2 = Scatter(
        lambda i, b: dot(GPRE[rows_of(i, 256), :], WF1[at(b * 256, 256), :], NT),
        SA, SAR, YA, YAR, ACCA,
    )
    phase("p22_rsh2")
    rs_h2.launch()

    x1, x2, xq, xo = sem(4), sem(4), sem(3), sem()

    half = ndp // 2
    upper = d >= half
    inward = jnp.where(upper, d - 1, d + 1)
    outward = jnp.where(upper, (d + 1) % ndp, (d + ndp - 1) % ndp)
    pos = jnp.where(upper, ndp - 1 - d, d)
    dev_in, dev_out = (inward, r, c), (outward, r, c)

    class Piece:
        def __init__(self, plan, xsend, xrecv, xs, send, recv, across, regions, steps, block, place):
            self.plan = list(plan)
            self.xsend, self.xrecv, self.xs = xsend, xrecv, xs
            self.send, self.recv, self.across, self.regions = send, recv, across, regions
            self.steps, self.block, self.place = steps, block, place
            self.s, self.c, self.g, self.a, self.l = sem(), sem(), sem(len(regions)), sem(4), lsem()
            self.state = 0

        def add(self, other):
            count_, cut = self.steps

            def one(i):
                k = cut(i)
                self.send[k] = (self.send[k].astype(f32) + other[k].astype(f32)).astype(bf16)

            loop(count_, one)

        def spread(self):
            lc(self.block(c), self.place(c), self.l).start()
            if self.a is not None:
                for rel, (to, dev) in enumerate(relations):
                    rc(self.block(to), self.place(c), self.a + rel, dev).start()

        def spread_wait(self):
            lc(self.block(c), self.place(c), self.l).wait()
            if self.a is not None:
                for rel, (cs, dev) in enumerate(relations):
                    rc(self.block(cs), self.place(cs), self.a + rel, dev).wait()
            for n, region in enumerate(self.regions):
                rc(region, region, self.g + n, dev_out).start()

        def step(self):
            k = self.state
            self.state += 1
            up = rc(self.send, self.recv, self.s, dev_in)
            cross = rc(self.send, self.across, self.c, dev_in)
            if k == 0:
                rc(self.xsend, self.xrecv, self.xs, dev_x).wait()
                self.add(self.xrecv)
                for t in range(half - 1):

                    @pl.when(pos == t)
                    def _():
                        if t > 0:
                            up.wait_recv()
                            self.add(self.recv)
                        up.start()

            elif k == 1:

                @pl.when(pos == half - 1)
                def _():
                    up.wait_recv()
                    self.add(self.recv)
                    cross.start()

            elif k == 2:

                @pl.when(pos == half - 1)
                def _():
                    cross.wait()
                    self.add(self.across)
                    self.spread()

            elif k == 3:
                pl.when(pos == half - 1)(self.spread_wait)
            else:
                outs = [rc(a, a, self.g + n, dev_out) for n, a in enumerate(self.regions)]

                for t in range(half - 2, -1, -1):

                    @pl.when(pos == t)
                    def _():
                        for out in outs:
                            out.wait_recv()
                            if t > 0:
                                out.start()

                @pl.when(pos > 0)
                def _():
                    for out in outs:
                        out.wait_send()

                pl.when(pos < half - 1)(up.wait_send)

    pieces = []
    for n in range(4):
        k = (n // 2, slice(None), pl.ds(128 * (n % 2), 128), slice(None))
        pieces.append(
            Piece(
                PLAN[n],
                X1S.at[k], X1R.at[k], x1 + n, ZS1.at[k], ZR1.at[k], ZC1.at[k],
                [g1_o.at[k[2], pl.ds(512 * cs + 256 * k[0], 256)] for cs in range(4)], (4, lambda i: i),
                lambda c2, k=k: ZS1.at[k[0], c2, k[2], :],
                lambda cs, k=k: g1_o.at[k[2], at(cs * 512 + 256 * k[0], 256)],
            )
        )
    for n in range(4):
        b = pl.ds(128 * n, 128)
        pieces.append(
            Piece(
                PLAN[4 + n],
                X2S.at[b], X2R.at[b], x2 + n, ZS2.at[b], ZR2.at[b], ZC2.at[b],
                [g2_o.at[:, b, :]], (4, lambda i: (rows_of(i, 32), slice(None))),
                lambda c2, b=b: ZS2.at[b, at(256 * c2, 256)],
                lambda cs, b=b: g2_o.at[cs, b, :],
            )
        )
    piece_o = Piece(
        PLAN[8],
        XOS, XOR, xo, ZSO, ZRO, ZCO,
        [go_o], (4, lambda i: (rows_of(i, 128), slice(None))),
        lambda c2: ZSO, lambda cs: go_o,
    )
    piece_o.a = None
    pieces.append(piece_o)
    for n in range(3):
        pieces.append(
            Piece(
                PLAN[9 + n],
                XQS.at[n], XQR.at[n], xq + n, ZSQ.at[n], ZRQ.at[n], ZCQ.at[n],
                [gq_o.at[n]], (4, lambda i: i),
                lambda c2, n=n: ZSQ.at[n, c2],
                lambda cs, n=n: gq_o.at[n, :, at(128 * cs, 128)],
            )
        )

    def tick(now):
        due = sorted((p.plan[k], n, k) for n, p in enumerate(pieces) for k in range(p.state, 4) if p.plan[k] <= now)
        for _, n, k in due:
            assert pieces[n].state == k
            if now > 900:
                phase(f"p52_{n:02d}_{k}")
            pieces[n].step()

    def dw1_half(p):
        def step(i):
            h = H2[:, rows_of(i, 256)]
            X1S[p, i] = dot(h, GPRE[:, at(512 * q_ + 256 * p, 256)], TN).astype(bf16)
            ZS1[p, i] = dot(h, GPRE[:, at(512 * r + 256 * p, 256)], TN).astype(bf16)

        loop(4, step)
        for n in range(2):
            b = pl.ds(128 * n, 128)
            rc(X1S.at[p, :, b, :], X1R.at[p, :, b, :], x1 + 2 * p + n, dev_x).start()

    phase("p23_dw1")
    dw1_half(0)
    dw1_half(1)

    rs_out = Scatter(
        lambda i, b: dot(ACT[rows_of(i, 256), :], WF2[:, at(b * 256, 256)], NN),
        SC, SCR, YC, YCR, ACCA,
    )

    def dw2_step(i):
        rows = rows_of(i, 256)
        X2S[rows, :] = dot(ACT[:, at(512 * q_ + 256 * i, 256)], GM[...], TN).astype(bf16)
        for n in range(2):
            block = at(256 * i + 128 * n, 128)
            rc(X2S.at[block], X2R.at[block], x2 + 2 * i + n, dev_x).start()
        ZS2[rows, :] = dot(ACT[:, at(512 * r + 256 * i, 256)], GM[...], TN).astype(bf16)

    phase("p25_dw2")
    loop(2, dw2_step)
    tick(92)

    def b2_sums(i):
        value = rs_h2.four(i)
        ACCA[rows_of(i, 256), :] = value
        for s in range(2):
            rows = at(i * 256 + s * 128, 128)
            gh, normed = ACCA[rows, :], N2[rows, :]
            add_to(G_SHIFT2, token_sum(gh))
            hn = gh * normed
            add_to(G_SCALE2, token_sum(hn))
            st3.put(
                2 * i + s,
                jnp.sum(gh * scale(2), axis=1, keepdims=True),
                jnp.sum(hn * scale(2), axis=1, keepdims=True),
            )

    phase("p26_b2sums")
    loop(4, b2_sums)
    st3.exchange()
    phase("p27_b2stat")
    s1, s2 = st3.total()
    CV[4] = s1 / D
    CV[5] = s2 / D

    def b2_back(i):
        rows = rows_of(i, 128)
        inner = ACCA[rows, :] * scale(2) - column(4, i) - N2[rows, :] * column(5, i)
        gmid = COT[rows, :] + column(3, i) * inner
        N2[rows, :] = gmid
        ga = gmid * gate(1)
        add_to((6, 0), token_sum(ga))
        add_to(G_GATE1, token_sum(gmid * ATT[rows, :]))
        GA[rows, :] = ga.astype(bf16)

    def out_done(i):
        value = rs_out.four(i) + bfc2[...]
        rows = rows_of(i, 256)
        add_to(G_GATE2, token_sum(COT[rows, :] * value))
        X[rows, :] = X[rows, :] + gate(2) * value

    phase("p29_b2back")
    loop(8, b2_back)
    tick(97)
    rs_mix = Scatter(
        lambda i, b: dot(GA[rows_of(i, 256), :], WOUT[at(b * 256, 256), :], NT),
        SC, SCR, YC, YCR, ACCA,
    )
    phase("p30_rsmix")
    loop(4, rs_mix.one)
    loop(4, rs_mix.two)
    tick(100)
    loop(4, rs_mix.three)

    def dwo_step(i):
        rows = rows_of(i, 128)
        XOS[rows, :] = dot(MIX[:, at(256 * i + 128 * q_, 128)], GA[...], TN).astype(bf16)
        ZSO[rows, :] = dot(MIX[:, at(256 * i + 128 * r, 128)], GA[...], TN).astype(bf16)

    phase("p31_dwo")
    loop(4, dwo_step)
    rc(XOS, XOR, xo, dev_x).start()
    tick(103)

    def do_step(i):
        DO[rows_of(i, 256), :] = rs_mix.four(i).astype(bf16)

    def inner_step(i):
        rows = rows_of(i, 128)
        prod = DO[rows, :].astype(f32) * MIX[rows, mine].astype(f32)
        lane = lax.broadcasted_iota(jnp.int32, (128, 256), 1) // HD
        inner = jnp.zeros((128, 128), f32)
        for h in range(4):
            one = jnp.sum(jnp.where(lane == h, prod, 0.0), axis=1, keepdims=True)
            inner = jnp.where(lane128 == h, one, inner)
        I8[:, rows] = inner.T[0:8, :]
        L8[:, rows] = LT[rows, :].T[0:8, :]

    def kt_step(i):
        rows = rows_of(i, 256)
        KT[:, rows] = K[rows, :].astype(f32).T.astype(bf16)

    phase("p33_kt")
    loop(4, kt_step)
    BQV[...] = jnp.zeros_like(BQV)
    phase("p34_do")
    for i in range(4):
        do_step(i)
        tick(105 + 2.5 * i)
    phase("p35_inner")
    loop(8, inner_step)
    lane_all = lax.broadcasted_iota(jnp.int32, (1024, 256), 1) // HD

    def head_back(n, half, now):
        h = 2 * half + n
        QM[...] = jnp.where(lane_all == h, Q[...], jnp.zeros_like(Q[...]))
        DOM[...] = jnp.where(lane_all == h, DO[...], jnp.zeros_like(DO[...]))
        feats = at(h * HD, HD)
        lanes = at(half * 128, 128)

        def step(i, first):
            rows = rows_of(i, 512)
            p = jnp.exp2(dot(K[rows, :], QM[...], NT) * (FACTOR * LOG2E) - L8[pl.ds(h, 1), :])
            dp = dot(V[rows, :], DOM[...], NT)
            ds = (p * (dp - I8[pl.ds(h, 1), :])).astype(bf16)
            gv = dot(p.astype(bf16), DOM[:, lanes], NN)
            gk = dot(ds, QM[:, lanes], NN)
            if n == 0:
                DV[rows, lanes] = gv
                DK[rows, lanes] = gk
            else:
                DV[rows, lanes] += gv
                DK[rows, lanes] += gk
            gq = dot(KT[feats, rows], ds, NN)

            if first:
                DQT[feats, :] = gq
            else:
                DQT[feats, :] += gq

        step(0, True)
        step(1, False)
        tick(now)

    def gqkv_half(half):
        feats, lanes = at(128 * half, 128), at(128 * half, 128)

        def step(i):
            rows = rows_of(i, 256)
            gq = DQT[feats, rows].T * FACTOR
            gk, gv = DK[rows, lanes] * FACTOR, DV[rows, lanes]
            BQV[half, 0:1, :] += token_sum(gq)
            BQV[half, 1:2, :] += token_sum(gv)
            GQKV[0, rows, lanes] = gq.astype(bf16)
            GQKV[1, rows, lanes] = gk.astype(bf16)
            GQKV[2, rows, lanes] = gv.astype(bf16)

        loop(4, step)

    def dwq_half(half, out, j):
        lanes = at(128 * half, 128)

        def step(i):
            out[j, i] = dot(H1[:, rows_of(i, 256)], GQKV[j, :, lanes], TN).astype(bf16)

        loop(4, step)

    phase("p36_head0")
    head_back(0, q_, 116)
    tick(117.5)
    phase("p36_head1")
    head_back(1, q_, 119)
    gqkv_half(q_)
    phase("p37_dwq0")
    for j in range(3):
        dwq_half(q_, XQS, j)
        rc(XQS.at[j], XQR.at[j], xq + j, dev_x).start()
        tick(122.5 + 1.5 * j)
    phase("p38_head2")
    head_back(0, r, 127)
    tick(128.5)
    phase("p39_head3")
    head_back(1, r, 130)
    gqkv_half(r)
    tick(131.5)

    def part_h1(i, b):
        rows, feats = rows_of(i, 256), at(b * 256, 256)
        total = dot(GQKV[0, rows, :], WQ[0, feats, :], NT)
        total = total + dot(GQKV[1, rows, :], WQ[1, feats, :], NT)
        return total + dot(GQKV[2, rows, :], WQ[2, feats, :], NT)

    phase("p43_rsh1")
    rs_h2.drain()
    rs_h1 = Scatter(part_h1, SA, SAR, YA, YAR, ACCA)
    loop(4, rs_h1.one)
    loop(4, rs_h1.two)
    phase("p44_three")
    loop(4, rs_h1.three)
    tick(136)
    phase("p44_dwq1")
    for j in range(3):
        dwq_half(r, ZSQ, j)
        tick(138 + 1.5 * j)

    def b1_sums(i):
        value = rs_h1.four(i)
        ACCA[rows_of(i, 256), :] = value
        for s in range(2):
            rows = at(i * 256 + s * 128, 128)
            gh, normed = ACCA[rows, :], N1[rows, :]
            add_to(G_SHIFT1, token_sum(gh))
            hn = gh * normed
            add_to(G_SCALE1, token_sum(hn))
            st4.put(
                2 * i + s,
                jnp.sum(gh * scale(1), axis=1, keepdims=True),
                jnp.sum(hn * scale(1), axis=1, keepdims=True),
            )

    phase("p48_b1sums")
    for i in range(4):
        b1_sums(i)
        tick(142.5 + 1.5 * i)
    st4.exchange()
    tick(148)
    phase("p50_b1stat")
    s1, s2 = st4.total()
    CV[6] = s1 / D
    CV[7] = s2 / D

    def b1_back(i):
        rows = rows_of(i, 128)
        inner = ACCA[rows, :] * scale(1) - column(6, i) - N1[rows, :] * column(7, i)
        N2[rows, :] = N2[rows, :] + column(1, i) * inner

    phase("p51_b1back")
    loop(8, b1_back)
    put_grad = lc(N2, gin_o, lsem())
    put_grad.start()
    finals.append(put_grad.wait)
    tick(151)
    tick(168)
    phase("p51_rsout")
    rs_mix.drain()
    loop(4, rs_out.one)
    loop(4, rs_out.two)
    tick(1000)
    phase("p51_out")
    loop(4, rs_out.three)
    for i in range(4):
        out_done(i)
    put_result = lc(X, res_o, lsem())
    put_result.start()
    finals.append(put_result.wait)
    SVL[5:6, 0:128] = BQV[0, 0:1, :]
    SVL[5:6, 128:256] = BQV[1, 0:1, :]
    SVL[5:6, 256:384] = BQV[0, 1:2, :]
    SVL[5:6, 384:512] = BQV[1, 1:2, :]
    SVA[me] = SVL[...]
    sva = ToAll(SVA)
    sva.start()

    phase("p52_ticks")
    tick(1000)

    phase("p56_sva")
    aca.wait()
    sva.wait()
    total = jnp.zeros((8, 512), f32)
    for l in range(nl):
        one = SVA[l]
        total = total + one
        act_o[l] = ACA[l]
        for k in range(6):
            gm_o[l, k : k + 1, :] = one[2 + k // 2 : 3 + k // 2, 256 * (k % 2) : 256 * (k % 2) + 256]
        gm_o[l, 6:8, :] = jnp.zeros((2, 256), f32)
    gmo_o[...] = gm_o[me]
    first = r == 0
    for k in range(6):
        gbada_o[k : k + 1, :] = total[2 + k // 2 : 3 + k // 2, 256 * (k % 2) : 256 * (k % 2) + 256]
    gbfc1_o[...] = jnp.where(first, total[0:1, :], total[1:2, :])
    gbqv_o[0:1, :] = jnp.where(first, total[5:6, 0:128], total[5:6, 128:256])
    gbqv_o[1:2, :] = jnp.where(first, total[5:6, 256:384], total[5:6, 384:512])
    gbout_o[...] = total[6:7, 0:256]
    gbfc2_o[...] = total[6:7, 256:512]

    phase("p57_finals")
    rs_out.drain()
    rs_h1.drain()
    for one in finals:
        one()
    phase("p58_pieces")
    for n, one in enumerate(pieces):
        phase(f"p59_{n:02d}")
        one.step()
    phase("")


def call_mega(ndp, *args):
    nl = 2 * ndp
    s = jax.ShapeDtypeStruct
    vmem = pl.BlockSpec(memory_space=pltpu.VMEM)
    hbm = pl.BlockSpec(memory_space=pl.ANY)
    outs = (
        (s((T, 256), f32), hbm),
        (s((T, 256), f32), hbm),
        (s((3, 256, 512), bf16), hbm),
        (s((512, 256), bf16), hbm),
        (s((256, 2048), bf16), hbm),
        (s((4, 512, 256), bf16), hbm),
        (s((nl, 8, 256), f32), vmem),
        (s((nl, 8, 128), f32), vmem),
        (s((8, 256), f32), vmem),
        (s((2, 128), f32), vmem),
        (s((1, 512), f32), vmem),
        (s((1, 256), f32), vmem),
        (s((1, 256), f32), vmem),
        (s((6, 256), f32), vmem),
    )

    def v(*shape, t=bf16):
        return pltpu.VMEM(shape, t)

    scratch = (
        [v(T, 256, t=f32)] * 5
        + [v(3, D, 256), v(D, 256), v(D, D), v(D, D)]
        + [v(T, D)] * 4
        + [v(T, 256)] * 3
        + [v(256, T), v(T, 128, t=f32), v(8, T, t=f32), v(8, T, t=f32)]
        + [v(T, 256)]
        + [v(T, D)] * 2
        + [v(T, 512), v(T, 512), v(T, 256), v(T, 256)] * 2
        + [v(T, 256, t=f32)]
        + [v(256, T, t=f32), v(T, 256, t=f32), v(T, 256, t=f32), v(T, 256), v(T, 256), v(3, T, 256)]
        + [v(2, 4, 256, 256)] * 5
        + [v(512, D)] * 5
        + [v(3, 4, 256, 128)] * 5
        + [v(512, 256)] * 5
        + [v(4, 4, 16, 128, t=f32), v(8, 8, 128, t=f32), v(2, 8, 512, t=f32), v(8, 512, t=f32)]
        + [v(nl, 8, 512, t=f32), v(nl, 8, 128, t=f32), v(2, 8, 128, t=f32)]
        + [pltpu.SemaphoreType.DMA((N_SEM + 16 * ndp,))] * 2
        + [pltpu.SemaphoreType.DMA((40,))]
    )
    return pl.pallas_call(
        functools.partial(mega, ndp),
        out_shape=[o[0] for o in outs],
        in_specs=[hbm] * 6 + [vmem] * 6,
        out_specs=[o[1] for o in outs],
        scratch_shapes=scratch,
        name="block",
        compiler_params=pltpu.CompilerParams(
            collective_id=0, has_side_effects=True, vmem_limit_bytes=67043328
        ),
    )(*args)


def body(
    inputs, cond, w_ada, b_ada, w_qkv, b_qv, w_out, b_out, w_fc1, b_fc1, w_fc2, b_fc2, cotangent
):
    assert cond.shape[0] == 1 and inputs.shape == (T, 256)
    ndp = lax.axis_size("dp")
    act_cond = jax.nn.silu(cond).astype(bf16)
    modulation = (
        jnp.einsum("sd,dke->ske", act_cond, w_ada, preferred_element_type=f32) + b_ada[None]
    )[0]
    mod8 = jnp.concatenate([modulation, jnp.zeros((2, 256), f32)], axis=0)
    actb = act_cond.astype(f32).reshape(8, 128)
    (
        result, grad_inputs, gq, go, g1, g2, gm, act_all, gmo, gbqv, gbfc1, gbout, gbfc2, gbada,
    ) = call_mega(
        ndp, inputs, cotangent, w_qkv, w_out, w_fc1, w_fc2, mod8, actb,
        b_qv, b_out[None], b_fc1[None], b_fc2[None],
    )
    parts = []
    rest = gm[:, :6]
    for _ in range(3):
        parts.append(lax.reduce_precision(rest, 8, 7))
        rest = rest - parts[-1]
    cut = jnp.concatenate(parts, axis=0).astype(bf16)
    act_low = jnp.concatenate([act_all.reshape(-1, D)] * 3, axis=0).astype(bf16)
    grad_w_ada = jnp.einsum("ld,lke->dke", act_low, cut, preferred_element_type=f32)
    parts = []
    rest = gmo[:6]
    for _ in range(3):
        parts.append(lax.reduce_precision(rest, 8, 7))
        rest = rest - parts[-1]
    own = jnp.stack(parts).astype(bf16)
    grad_silu = lax.psum(
        jnp.sum(
            jnp.einsum("pke,dke->pd", own, w_ada, preferred_element_type=f32),
            axis=0,
            keepdims=True,
        ),
        "col",
    )
    grad_cond = jax.vjp(jax.nn.silu, cond)[1](grad_silu)[0]
    return (
        result,
        grad_inputs,
        grad_cond,
        grad_w_ada,
        gbada,
        gq.astype(f32),
        gbqv,
        go.astype(f32),
        gbout[0],
        g1.astype(f32),
        gbfc1[0],
        g2.reshape(2048, 256).astype(f32),
        gbfc2[0],
    )


def solution(mesh):
    return jax.shard_map(
        body,
        mesh=mesh,
        in_specs=(
            P(("dp", "row"), "col"),
            P(("dp", "row"), None),
            P(None, None, "col"),
            P(None, "col"),
            P(None, "col", "row"),
            P(None, ("row", "col")),
            P("row", "col"),
            P("col"),
            P("col", "row"),
            P(("row", "col")),
            P("row", "col"),
            P("col"),
            P(("dp", "row"), "col"),
        ),
        out_specs=(
            P(("dp", "row"), "col"),
            P(("dp", "row"), "col"),
            P(("dp", "row"), None),
            P(None, None, "col"),
            P(None, "col"),
            P(None, "col", "row"),
            P(None, ("row", "col")),
            P("row", "col"),
            P("col"),
            P("col", "row"),
            P(("row", "col")),
            P("row", "col"),
            P("col"),
        ),
        check_vma=False,
    )
```
